256 devices in a mesh: row: 32 (over y, z), col: 8 (over x, core).
Axes of the slice: x: 4, y: 4, z: 8, core: 2. Of those that a mesh axis runs over, the one named last changes fastest.
Arguments:
- points: float32 [16, 32768], P(None, ('col', 'row')), may hold values from -5 to 5
- inv_scales: float32 [16], replicated, may hold values from 0.1 to 0.4
- amplitude: float32 [1], replicated, may hold values from 0.5 to 2
- noise_var: float32 [1], replicated, may hold values from 0.3 to 1
- targets: float32 [8, 32768], P(None, ('col', 'row')), may hold values from -6 to 6
- initial: float32 [8, 32768], P(None, ('col', 'row')), may hold values from -3 to 3
- ritz_basis: float32 [64, 32768], P(None, ('col', 'row')), may hold values from -0.03125 to 0.03125
Outputs:
- solution: float32 [8, 32768], P(None, ('col', 'row'))
- residual: float32 [8, 32768], P(None, ('col', 'row'))
The draws below stay inside these ranges and needn't reach their ends.
All inputs are finite; a program needn't handle non-finite values.
Results may differ from the reference program's by a relative error of at most 0.00065.
Values sent between devices are 32-bit elements; how exact they have to be, the bound alone decides.
A program may use at most 128 MiB of HBM per device.

```python
import math
import jax
import jax.numpy as jnp
from jax import lax

FEAT = 16
RITZ = 64
ITERS = 1
RHS = 8
POINTS = 32768


def level_of(key, dims, cuts, low, largest):
    level = 1.0
    for axis_at, parts in cuts:
        draws = jax.random.uniform(jax.random.fold_in(jax.random.fold_in(key, 6), axis_at), (parts,), jnp.float32, low / len(cuts), largest / len(cuts))
        level = level * jnp.repeat(jnp.exp(draws), dims[axis_at] // parts).reshape((-1,) + (1,) * (len(dims) - 1 - axis_at))
    return level


def normal_values(key, extent, deviation, reach, split=(), kind=jnp.bfloat16):
    level = level_of(key, extent, split, -0.22, 0.18) if split else 1.0
    drawn = jax.random.normal(key, extent, jnp.float32) * deviation * level
    return jnp.minimum(jnp.maximum(drawn, -reach), reach).astype(kind)


def setup_inputs(seed: int = 0) -> dict:
    key_list = jax.random.split(jax.random.key(seed), 8)
    points = normal_values(key_list[0], (FEAT, POINTS), 1.0, 5.0, ((1, 256),), jnp.float32)
    inv_scales = jnp.clip(jnp.exp(jax.random.uniform(key_list[1], (FEAT,), jnp.float32, math.log(0.1), math.log(0.4))), 0.1, 0.4)
    amplitude = jnp.clip(jnp.exp(jax.random.uniform(key_list[2], (1,), jnp.float32, math.log(0.5), math.log(2.0))), 0.5, 2.0)
    noise_var = jnp.clip(jnp.exp(jax.random.uniform(key_list[3], (1,), jnp.float32, math.log(0.3), math.log(1.0))), 0.3, 1.0)
    targets = normal_values(key_list[4], (RHS, POINTS), 1.0, 6.0, ((1, 256),), jnp.float32)
    initial = normal_values(key_list[5], (RHS, POINTS), 0.5, 3.0, ((1, 256),), jnp.float32)
    ritz_basis = normal_values(key_list[6], (RITZ, POINTS), POINTS ** -0.5, 0.03125, ((1, 256),), jnp.float32)
    return dict(points=points, inv_scales=inv_scales, amplitude=amplitude, noise_var=noise_var, targets=targets, initial=initial, ritz_basis=ritz_basis)


HIGH = lax.Precision.HIGHEST

def kernel_tile(col_x, col_sq, row_x, row_sq, gain):
    cross_term = jnp.dot(col_x.T.astype(jnp.float32), row_x.astype(jnp.float32), precision=HIGH, preferred_element_type=jnp.float32)
    distance = jnp.maximum(col_sq[:, None] + row_sq[None, :] - 2.0 * cross_term, 0.0)
    return gain * jnp.exp(-0.5 * distance)

def coarse_solve(factor, rhs_block):
    middle = lax.linalg.triangular_solve(factor, rhs_block, left_side=True, lower=True)
    return lax.linalg.triangular_solve(factor, middle, left_side=True, lower=True, transpose_a=True)

def matmul(left, right):
    return jnp.dot(left.astype(jnp.float32), right.astype(jnp.float32), precision=HIGH, preferred_element_type=jnp.float32)

def apply_operator(vectors, scaled, sq_norms, gain, nugget):
    length = scaled.shape[1]
    block_size = math.gcd(length, 2048)
    num_blocks = length // block_size

    def one_block(block_index):
        offset = (block_index * block_size).astype(jnp.int32)
        row_x = lax.dynamic_slice_in_dim(scaled, offset, block_size, 1)
        row_sq = lax.dynamic_slice_in_dim(sq_norms, offset, block_size, 0)
        kernel_block = kernel_tile(scaled, sq_norms, row_x, row_sq, gain)
        return jnp.dot(vectors.astype(jnp.float32), kernel_block.astype(jnp.float32), precision=HIGH, preferred_element_type=jnp.float32)
    results = lax.map(one_block, jnp.arange(num_blocks, dtype=jnp.int32))
    results = jnp.transpose(results, (1, 0, 2)).reshape(vectors.shape[0], length)
    return results + nugget * vectors

def reference(points, inv_scales, amplitude, noise_var, targets, initial, ritz_basis):
    gain = amplitude[0]
    nugget = noise_var[0]
    scaled = points * inv_scales[:, None]
    sq_norms = jnp.sum(scaled * scaled, axis=0)
    rhs_count = initial.shape[0]
    applied_all = apply_operator(jnp.concatenate([initial, ritz_basis], 0), scaled, sq_norms, gain, nugget)
    ritz_image = applied_all[rhs_count:]
    first_residual = targets - applied_all[:rhs_count]
    coarse = matmul(ritz_basis, ritz_image.T)
    coarse = 0.5 * (coarse + coarse.T)
    projected = matmul(ritz_basis, first_residual.T)
    factor = jnp.linalg.cholesky(coarse)
    coarse_inverse = coarse_solve(factor, jnp.eye(coarse.shape[0], dtype=coarse.dtype))
    amounts = matmul(coarse_inverse, projected)
    solution = initial + matmul(amounts.T, ritz_basis)
    residual = first_residual - matmul(amounts.T, ritz_image)
    against = matmul(ritz_image, residual.T)
    sq_norm = jnp.sum(residual * residual, axis=1)
    direction = residual - matmul(matmul(coarse_inverse, against).T, ritz_basis)
    for step in range(ITERS):
        applied = apply_operator(direction, scaled, sq_norms, gain, nugget)
        step_size = sq_norm / jnp.sum(direction * applied, axis=1)
        solution = solution + step_size[:, None] * direction
        residual = residual - step_size[:, None] * applied
        against = matmul(ritz_image, residual.T)
        new_norm = jnp.sum(residual * residual, axis=1)
        correction = matmul(matmul(coarse_inverse, against).T, ritz_basis)
        direction = residual + (new_norm / sq_norm)[:, None] * direction - correction
        sq_norm = new_norm
    return (solution, residual)
```

```python
import functools
import math

import jax
import jax.numpy as jnp
from jax import lax
from jax.experimental import pallas as pl
from jax.experimental.pallas import tpu as pltpu
from jax.sharding import Mesh
from jax.sharding import PartitionSpec as P

F32 = jnp.float32
BF16 = jnp.bfloat16
HIGH = lax.Precision.HIGHEST
MESH = pl.DeviceIdType.MESH
NY, NZ, NX, NC = 4, 8, 4, 2
NF = NX * NY * NC
NG = NX * NC
NQ = NY * NZ
BLK = 128
FEAT = 16
RITZ = 64
RHS = 8
VEC = RITZ + RHS
PAD = 80
NJ = NF * BLK
NPAIR = NZ // 2
STEPS = 16
CHUNK = NJ * NPAIR // STEPS
PER_PAIR = NJ // CHUNK
LOG2E = 1.4426950408889634


def split3(a):
    high = a.astype(BF16).astype(F32)
    rest = a - high
    mid = rest.astype(BF16).astype(F32)
    low = (rest - mid).astype(BF16).astype(F32)
    return high, mid, low


def matmul(a, b, dims):
    return lax.dot_general(a, b, (dims, ((), ())), precision=HIGH, preferred_element_type=F32)


def fast(a, b):
    return jnp.dot(a, b, preferred_element_type=F32)


def features(y, left):
    h, m, low = split3(y)
    sh, sm, sl = split3(-0.5 * jnp.sum(y * y, axis=0, keepdims=True))
    row = lax.broadcasted_iota(jnp.int32, (FEAT, BLK), 0)
    at = 0 if left else 3
    ones = (row < 6) & ((row >= 3) if left else (row < 3))
    extra = jnp.where(row == at, sh, jnp.where(row == at + 1, sm, jnp.where(row == at + 2, sl, 0.0)))
    extra = jnp.where(ones, 1.0, extra)
    zero = jnp.zeros((FEAT, BLK), F32)
    parts = [h, m, h, low, h, m, extra, zero] if left else [h, h, m, h, low, m, extra, zero]
    return jnp.concatenate(parts, axis=0)


def body(
    gain_ref, nugget_ref, scales_ref, points_ref, targets_ref, initial_ref, ritz_ref, out_ref, res_ref,
    px, xf, xz, vf, wz, tgt, ljt, riz, khi, klo, vcat, part, pin, ars, ara, arb, arc, df, dz, fs, fr, gf, dcat,
    sem_in, rx, rxz, rv, rvf, rw, rp, ra, rb, rc, rd, rdz, rf, rg,
    sx, sxz, sv, svf, sw, sp, sa, sb, sc, sd, sdz, sf, sg,
):
    y = lax.axis_index("row_0")
    z = lax.axis_index("row_1")
    x = lax.axis_index("col_0")
    c = lax.axis_index("col_1")
    chip = x * NY + y
    f = chip * NC + c
    g = x * NC + c
    q = y * NZ + z

    def xyc(k):
        o = lax.rem(f + k, NF)
        return {"row_0": lax.rem(o // NC, NY), "row_1": z, "col_0": o // (NC * NY), "col_1": lax.rem(o, NC)}

    def at_z(o):
        return {"row_0": y, "row_1": o, "col_0": x, "col_1": c}

    def remote(src, dst, send, recv, device):
        return pltpu.make_async_remote_copy(
            src_ref=src, dst_ref=dst, send_sem=send, recv_sem=recv, device_id=device, device_id_type=MESH
        )

    def settle(ref, sem):
        pltpu.make_async_copy(ref, ref, sem).wait()

    loads = [
        pltpu.make_async_copy(points_ref, px, sem_in.at[0]),
        pltpu.make_async_copy(ritz_ref, vf.at[f, pl.ds(0, RITZ)], sem_in.at[1]),
        pltpu.make_async_copy(initial_ref, vf.at[f, pl.ds(RITZ, RHS)], sem_in.at[2]),
        pltpu.make_async_copy(targets_ref, tgt, sem_in.at[3]),
        pltpu.make_async_copy(ritz_ref, wz.at[:, pl.ds(pl.multiple_of(z * BLK, BLK), BLK)], sem_in.at[4]),
    ]
    for load in loads:
        load.start()
    barrier = pltpu.get_barrier_semaphore()

    @pl.loop(1, NF)
    def _(k):
        pl.semaphore_signal(barrier, inc=1, device_id=xyc(k), device_id_type=MESH)

    @pl.loop(1, NZ)
    def _(k):
        pl.semaphore_signal(barrier, inc=1, device_id=at_z(lax.rem(z + k, NZ)), device_id_type=MESH)

    gain = gain_ref[0]
    nugget = nugget_ref[0]
    row = lax.broadcasted_iota(jnp.int32, (FEAT, BLK), 0)
    scale = jnp.zeros((FEAT, BLK), F32)
    for i in range(FEAT):
        scale = jnp.where(row == i, scales_ref[i], scale)
    loads[0].wait()
    scaled = px[...] * scale * math.sqrt(LOG2E)
    xf[f] = scaled
    xz[z] = scaled
    for load in loads[1:]:
        load.wait()
    pl.semaphore_wait(barrier, NF - 1 + NZ - 1)

    @pl.loop(1, NF)
    def _(k):
        remote(xf.at[f], xf.at[f], sx, rx, xyc(k)).start()

    @pl.loop(1, NZ)
    def _(k):
        remote(xz.at[z], xz.at[z], sxz, rxz, at_z(lax.rem(z + k, NZ))).start()

    @pl.loop(1, NX * NY)
    def _(k):
        remote(vf.at[f], vf.at[f], sv, rv.at[k], xyc(k * NC)).start()

    own_w = wz.at[:, pl.ds(pl.multiple_of(z * BLK, BLK), BLK)]

    @pl.loop(1, NZ)
    def _(k):
        remote(own_w, own_w, sw, rw, at_z(lax.rem(z + k, NZ))).start()

    settle(xf.at[pl.ds(0, NF - 1)], rx)

    @pl.loop(0, NF)
    def _(j):
        ljt[pl.ds(pl.multiple_of(j * BLK, BLK), BLK), :] = features(xf[j], True).T.astype(BF16)

    settle(xz.at[pl.ds(0, NZ - 1)], rxz)
    for p in range(NPAIR):
        first = features(xz[lax.rem(z + NPAIR + p, NZ)], False)
        second = features(xz[lax.rem(z + NPAIR - 1 - p, NZ)], False)
        riz[p] = jnp.concatenate([first, second], axis=1).astype(BF16)

    other = {"row_0": y, "row_1": z, "col_0": x, "col_1": 1 - c}

    @pl.loop(0, STEPS)
    def _(i):
        p = i // PER_PAIR
        at = pl.ds(pl.multiple_of(lax.rem(i, PER_PAIR) * CHUNK, CHUNK), CHUNK)
        tile = jnp.exp2(jnp.minimum(fast(ljt[at, :], riz[p]), 0.0))
        high = tile.astype(BF16)
        khi[p, at, :] = high
        klo[p, at, :] = (tile - high.astype(F32)).astype(BF16)
        origin = lax.rem(f + NF - i * NC, NF)

        @pl.when(i > 0)
        def _():
            settle(vf.at[origin], rv.at[i])

        remote(vf.at[origin], vf.at[origin], svf, rvf, other).start()

    settle(vf.at[pl.ds(0, NF // NC)], rvf)

    @pl.loop(0, NF)
    def _(j):
        v = jnp.concatenate([vf[j], jnp.zeros((PAD - VEC, BLK), F32)], axis=0)
        h, m, low = split3(v)
        at = pl.ds(pl.multiple_of(j * BLK, BLK), BLK)
        vcat[0:PAD, at] = h.astype(BF16)
        vcat[PAD : 2 * PAD, at] = m.astype(BF16)
        vcat[2 * PAD : 3 * PAD, at] = low.astype(BF16)

    def block_at(o):
        return pl.ds(pl.multiple_of(o * BLK, BLK), BLK)

    own_vec = vf.at[f]

    @pl.loop(0, NPAIR)
    def _(p):
        a = fast(vcat[...], khi[p])
        b = fast(vcat[0 : 2 * PAD, :], klo[p])
        total = a[0:VEC] + a[PAD : PAD + VEC] + a[2 * PAD : 2 * PAD + VEC] + b[0:VEC] + b[PAD : PAD + VEC]
        total = total * gain
        first, second = lax.rem(z + NPAIR + p, NZ), lax.rem(z + NPAIR - 1 - p, NZ)
        part[:, block_at(first)] = total[:, :BLK]
        part[:, block_at(second)] = total[:, BLK:]
        remote(part.at[:, block_at(first)], pin.at[z], sp, rp, at_z(first)).start()

        @pl.when(p < NPAIR - 1)
        def _():
            remote(part.at[:, block_at(second)], pin.at[z], sp, rp, at_z(second)).start()

    mine = part[:, block_at(z)] + nugget * own_vec[...]
    part[:, block_at(z)] = mine
    pin[z] = mine

    def xc(k):
        o = lax.rem(g + k, NG)
        return o, {"row_0": y, "row_1": z, "col_0": o // NC, "col_1": lax.rem(o, NC)}

    def tile_at(o):
        return pl.ds(pl.multiple_of(o * RHS, RHS), RHS)

    def sum_a(n, value):
        ars[n] = value

        @pl.loop(1, NG)
        def _(k):
            o, device = xc(k)
            remote(ars.at[n, tile_at(o)], ara.at[n, g], sa.at[n], ra.at[n], device).start()

        ara[n, g] = ars[n, tile_at(g)]

    def sum_b(n):
        settle(ara.at[n, pl.ds(0, NG - 1)], ra.at[n])
        arb[n, q] = jnp.sum(ara[n], axis=0)

        @pl.loop(1, NQ)
        def _(k):
            o = lax.rem(q + k, NQ)
            device = {"row_0": o // NZ, "row_1": lax.rem(o, NZ), "col_0": x, "col_1": c}
            remote(arb.at[n, q], arb.at[n, q], sb.at[n], rb.at[n], device).start()

    def sum_c(n):
        settle(arb.at[n, pl.ds(0, NQ - 1)], rb.at[n])
        arc[n, g] = jnp.sum(arb[n], axis=0)

        @pl.loop(1, NG)
        def _(k):
            _, device = xc(k)
            remote(arc.at[n, g], arc.at[n, g], sc.at[n], rc.at[n], device).start()

    def sum_d(n):
        settle(arc.at[n, pl.ds(0, NG - 1)], rc.at[n])
        return arc[n].reshape(RITZ, BLK)

    lane = lax.broadcasted_iota(jnp.int32, (RITZ, BLK), 1)
    settle(wz.at[:, pl.ds(0, (NZ - 1) * BLK)], rw)
    fill = jnp.zeros((BLK - VEC, BLK * NZ), F32)
    coarse_part = matmul(wz[...], jnp.concatenate([part[...], fill], axis=0), ((1,), (1,)))
    ritz_own = own_vec[0:RITZ, :]
    start_own = own_vec[RITZ:VEC, :]
    target_rows = jnp.concatenate(
        [jnp.zeros((RITZ, BLK), F32), tgt[...], jnp.zeros((BLK - VEC, BLK), F32)], axis=0
    )
    coarse_part = jnp.where(lane < RITZ, coarse_part, -coarse_part) + matmul(ritz_own, target_rows, ((1,), (1,)))
    sum_a(0, coarse_part)
    sum_b(0)
    settle(pin.at[pl.ds(0, NZ - 1)], rp)
    image = jnp.sum(pin[...], axis=0)
    zimg = image[0:RITZ]
    r0 = tgt[...] - image[RITZ:VEC]
    both = jnp.concatenate([zimg, r0, jnp.zeros((BLK - VEC, BLK), F32)], axis=0)
    sum_a(1, matmul(zimg, both, ((1,), (1,))))
    sum_c(0)
    sum_b(1)
    first_sum = sum_d(0)
    square = jnp.concatenate([first_sum, jnp.zeros((BLK - RITZ, BLK), F32)], axis=0)
    coarse = 0.5 * (first_sum + square.T[0:RITZ])
    sub = lax.broadcasted_iota(jnp.int32, (RITZ, BLK), 0)
    work = jnp.where(lane < RITZ, jnp.where(lane == sub, 1.0, 0.0), pltpu.roll(coarse, RITZ, 1))

    def eliminate(work, begin, end):
        for k in range(begin, end):
            pivot_row = work[k : k + 1, :] / work[k : k + 1, RITZ + k : RITZ + k + 1]
            column = work[:, RITZ + k : RITZ + k + 1] - jnp.where(sub[:, 0:1] == k, 1.0, 0.0)
            work = work - column * pivot_row
        return work

    work = eliminate(work, 0, 48)
    sum_c(1)
    work = eliminate(work, 48, RITZ)
    inverse = work[:, 0:RITZ]
    amounts = matmul(inverse, first_sum, ((1,), (0,)))
    wide = jnp.concatenate([ritz_own, zimg], axis=1)
    moved = matmul(amounts, wide, ((0,), (0,)))[RITZ:VEC]
    sol = start_own + moved[:, 0:BLK]
    resid = r0 - moved[:, BLK:]
    second_sum = sum_d(1)
    against = second_sum - matmul(second_sum[:, 0:RITZ], amounts, ((1,), (0,)))
    beta = matmul(inverse, against, ((1,), (0,)))
    direction = resid - matmul(beta, ritz_own, ((0,), (0,)))[RITZ:VEC]
    df[f] = direction
    dz[z, 0:RHS] = direction
    dz[z, RHS:] = resid * resid

    @pl.loop(1, NF)
    def _(k):
        remote(df.at[f], df.at[f], sd, rd, xyc(k)).start()

    @pl.loop(1, NZ)
    def _(k):
        remote(dz.at[z], dz.at[z], sdz, rdz, at_z(lax.rem(z + k, NZ))).start()

    settle(df.at[pl.ds(0, NF - 1)], rd)

    @pl.loop(0, NF)
    def _(j):
        h, m, low = split3(df[j])
        dcat[:, block_at(j)] = jnp.concatenate([h, m, low, jnp.zeros_like(h)], axis=0).astype(BF16)

    settle(dz.at[pl.ds(0, NZ - 1)], rdz)

    @pl.loop(0, NPAIR)
    def _(p):
        a = fast(dcat[...], khi[p])
        b = fast(dcat[0:16, :], klo[p])
        total = (a[0:8] + a[8:16] + a[16:24] + b[0:8] + b[8:16]) * gain
        fs[lax.rem(z + NPAIR + p, NZ), 0:RHS] = total[:, :BLK]
        fs[lax.rem(z + NPAIR - 1 - p, NZ), 0:RHS] = total[:, BLK:]

    fs[z, 0:RHS] = fs[z, 0:RHS] + nugget * direction
    curve = jnp.zeros((RHS, BLK), F32)
    square_sum = jnp.zeros((RHS, BLK), F32)
    for o in range(NZ):
        curve = curve + fs[o, 0:RHS] * dz[o, 0:RHS]
        square_sum = square_sum + dz[o, RHS:]
    for o in range(NZ):
        fs[o, RHS:] = curve

    @pl.loop(1, NZ)
    def _(k):
        o = lax.rem(z + k, NZ)
        remote(fs.at[o], fr.at[z], sf, rf, at_z(o)).start()

    fr[z] = fs[z]
    settle(fr.at[pl.ds(0, NZ - 1)], rf)
    arrived = jnp.sum(fr[...], axis=0)
    applied, curve = arrived[0:RHS], arrived[RHS:]
    lanes = lax.broadcasted_iota(jnp.int32, (RHS, BLK), 1)
    curve = curve + pltpu.roll(curve, BLK // 2, 1)
    square_sum = square_sum + pltpu.roll(square_sum, BLK // 2, 1)
    gf[f] = jnp.where(lanes < BLK // 2, curve, square_sum)

    @pl.loop(1, NF)
    def _(k):
        remote(gf.at[f], gf.at[f], sg, rg, xyc(k)).start()

    settle(gf.at[pl.ds(0, NF - 1)], rg)
    both = jnp.sum(gf[...], axis=0)
    bottom = jnp.sum(jnp.where(lanes < BLK // 2, both, 0.0), axis=1, keepdims=True)
    top = jnp.sum(jnp.where(lanes < BLK // 2, 0.0, both), axis=1, keepdims=True)
    step = top / bottom
    out_ref[...] = sol + step * direction
    res_ref[...] = resid - step * applied

    settle(xf.at[pl.ds(0, NF - 1)], sx)
    settle(xz.at[pl.ds(0, NZ - 1)], sxz)
    settle(vf.at[pl.ds(0, NX * NY - 1)], sv)
    settle(vf.at[pl.ds(0, NX * NY)], svf)
    settle(wz.at[:, pl.ds(0, (NZ - 1) * BLK)], sw)
    settle(pin.at[pl.ds(0, NZ - 1)], sp)
    for n in range(2):
        settle(ara.at[n, pl.ds(0, NG - 1)], sa.at[n])
        settle(arb.at[n, pl.ds(0, NQ - 1)], sb.at[n])
        settle(arc.at[n, pl.ds(0, NG - 1)], sc.at[n])
    settle(df.at[pl.ds(0, NF - 1)], sd)
    settle(dz.at[pl.ds(0, NZ - 1)], sdz)
    settle(fr.at[pl.ds(0, NZ - 1)], sf)
    settle(gf.at[pl.ds(0, NF - 1)], sg)


def local(points, inv_scales, amplitude, noise_var, targets, initial, ritz_basis):
    dma = pltpu.SemaphoreType.DMA
    smem = pl.BlockSpec(memory_space=pltpu.SMEM)
    hbm = pl.BlockSpec(memory_space=pl.ANY)
    vmem = pl.BlockSpec(memory_space=pltpu.VMEM)
    return pl.pallas_call(
        body,
        out_shape=(jax.ShapeDtypeStruct((RHS, BLK), F32), jax.ShapeDtypeStruct((RHS, BLK), F32)),
        in_specs=[smem, smem, smem, hbm, hbm, hbm, hbm],
        out_specs=(vmem, vmem),
        scratch_shapes=[
            pltpu.VMEM((FEAT, BLK), F32),
            pltpu.VMEM((NF, FEAT, BLK), F32),
            pltpu.VMEM((NZ, FEAT, BLK), F32),
            pltpu.VMEM((NF, VEC, BLK), F32),
            pltpu.VMEM((RITZ, NZ * BLK), F32),
            pltpu.VMEM((RHS, BLK), F32),
            pltpu.VMEM((NJ, BLK), BF16),
            pltpu.VMEM((NPAIR, BLK, 2 * BLK), BF16),
            pltpu.VMEM((NPAIR, NJ, 2 * BLK), BF16),
            pltpu.VMEM((NPAIR, NJ, 2 * BLK), BF16),
            pltpu.VMEM((3 * PAD, NJ), BF16),
            pltpu.VMEM((VEC, NZ * BLK), F32),
            pltpu.VMEM((NZ, VEC, BLK), F32),
            pltpu.VMEM((2, RITZ, BLK), F32),
            pltpu.VMEM((2, NG, RHS, BLK), F32),
            pltpu.VMEM((2, NQ, RHS, BLK), F32),
            pltpu.VMEM((2, NG, RHS, BLK), F32),
            pltpu.VMEM((NF, RHS, BLK), F32),
            pltpu.VMEM((NZ, 2 * RHS, BLK), F32),
            pltpu.VMEM((NZ, 2 * RHS, BLK), F32),
            pltpu.VMEM((NZ, 2 * RHS, BLK), F32),
            pltpu.VMEM((NF, RHS, BLK), F32),
            pltpu.VMEM((4 * RHS, NJ), BF16),
            dma((5,)), dma, dma, dma((NX * NY,)), dma, dma, dma, dma((2,)), dma((2,)), dma((2,)), dma, dma, dma, dma,
            dma, dma, dma, dma, dma, dma, dma((2,)), dma((2,)), dma((2,)), dma, dma, dma, dma,
        ],
        compiler_params=pltpu.CompilerParams(
            collective_id=0, has_side_effects=True, vmem_limit_bytes=60 * 1024 * 1024
        ),
    )(amplitude, noise_var, inv_scales, points, targets, initial, ritz_basis)


def solution(mesh):
    torus = Mesh(mesh.devices.reshape(NY, NZ, NX, NC), ("row_0", "row_1", "col_0", "col_1"))
    split = P(None, ("col_0", "col_1", "row_0", "row_1"))
    return jax.shard_map(
        local,
        mesh=torus,
        in_specs=(split, P(), P(), P(), split, split, split),
        out_specs=(split, split),
        check_vma=False,
    )
```

```python
import functools
import math

import jax
import jax.numpy as jnp
from jax import lax
from jax.experimental import pallas as pl
from jax.experimental.pallas import tpu as pltpu
from jax.sharding import Mesh
from jax.sharding import PartitionSpec as P

F32 = jnp.float32
BF16 = jnp.bfloat16
HIGH = lax.Precision.HIGHEST
MESH = pl.DeviceIdType.MESH
NY, NZ, NX, NC = 4, 8, 4, 2
NF = NX * NY * NC
NG = NX * NC
NQ = NY * NZ
BLK = 128
FEAT = 16
RITZ = 64
RHS = 8
VEC = RITZ + RHS
PAD = 80
NJ = NF * BLK
CHIPS = NX * NY
HALF = CHIPS * BLK
ROWS = 1024
HOLD = False
NI = NZ * BLK
NEAR = (0, 1, 3, 2)
LOG2E = 1.4426950408889634


def split3(a):
    high = a.astype(BF16).astype(F32)
    rest = a - high
    mid = rest.astype(BF16).astype(F32)
    low = (rest - mid).astype(BF16).astype(F32)
    return high, mid, low


def matmul(a, b, dims):
    return lax.dot_general(a, b, (dims, ((), ())), precision=HIGH, preferred_element_type=F32)


def fast(a, b):
    return jnp.dot(a, b, preferred_element_type=F32)


def features(y, left):
    h, m, low = split3(y)
    sh, sm, sl = split3(-0.5 * jnp.sum(y * y, axis=0, keepdims=True))
    row = lax.broadcasted_iota(jnp.int32, (FEAT, BLK), 0)
    at = 0 if left else 3
    ones = (row < 6) & ((row >= 3) if left else (row < 3))
    extra = jnp.where(row == at, sh, jnp.where(row == at + 1, sm, jnp.where(row == at + 2, sl, 0.0)))
    extra = jnp.where(ones, 1.0, extra)
    zero = jnp.zeros((FEAT, BLK), F32)
    parts = [h, m, h, low, h, m, extra, zero] if left else [h, h, m, h, low, m, extra, zero]
    return jnp.concatenate(parts, axis=0)


def inverse2(m):
    a, b, e, d = m
    r = 1.0 / (a * d - b * e)
    return d * r, -b * r, -e * r, a * r


def multiply2(m, n):
    return (
        m[0] * n[0] + m[1] * n[2],
        m[0] * n[1] + m[1] * n[3],
        m[2] * n[0] + m[3] * n[2],
        m[2] * n[1] + m[3] * n[3],
    )


def eliminate(work):
    def full(a):
        return jnp.broadcast_to(a, (RHS, BLK))

    sub = lax.broadcasted_iota(jnp.int32, (RHS, BLK), 0)
    tiles = [work[RHS * i : RHS * (i + 1)] for i in range(RITZ // RHS)]
    for k in range(0, RITZ, 4):
        v, r = k // RHS, k % RHS
        cols = [[full(t[:, RITZ + k + j : RITZ + k + j + 1]) for t in tiles] for j in range(4)]
        u = [full(tiles[v][r + i : r + i + 1]) for i in range(4)]
        m = [[full(cols[j][v][r + i : r + i + 1]) for j in range(4)] for i in range(4)]
        b = (m[0][2], m[0][3], m[1][2], m[1][3])
        first = inverse2((m[0][0], m[0][1], m[1][0], m[1][1]))
        low = multiply2((m[2][0], m[2][1], m[3][0], m[3][1]), first)
        schur = tuple(p - q for p, q in zip((m[2][2], m[2][3], m[3][2], m[3][3]), multiply2(low, b)))
        second = inverse2(schur)
        t2 = u[2] - low[0] * u[0] - low[1] * u[1]
        t3 = u[3] - low[2] * u[0] - low[3] * u[1]
        n2 = second[0] * t2 + second[1] * t3
        n3 = second[2] * t2 + second[3] * t3
        t0 = u[0] - b[0] * n2 - b[1] * n3
        t1 = u[1] - b[2] * n2 - b[3] * n3
        n0 = first[0] * t0 + first[1] * t1
        n1 = first[2] * t0 + first[3] * t1
        for j in range(4):
            cols[j][v] = jnp.where(sub == r + j, cols[j][v] - 1.0, cols[j][v])
        tiles = [
            t - (cols[0][i] * n0 + cols[1][i] * n1) - (cols[2][i] * n2 + cols[3][i] * n3)
            for i, t in enumerate(tiles)
        ]
    return jnp.concatenate(tiles, axis=0)


def body(
    gain_ref, nugget_ref, scales_ref, points_ref, targets_ref, initial_ref, ritz_ref, out_ref, res_ref,
    px, xf, xz, vf, wz, tgt, ljt, riz, khi, klo, vcat, part, pin, ars, ara, arb, arc, rf, rz, tz, tf, acc, fs, fr, gf,
    sem_in, rx, rxf, rxz, rv, rvf, rw, rp, ra, rb, rc, rr, rrz, rtz, rt, rs, rg,
    sx, sxf, sxz, sv, svf, sw, sp, sa, sb, sc, sr, srz, stz, st, ss, sg,
):
    y = lax.axis_index("row_0")
    z = lax.axis_index("row_1")
    x = lax.axis_index("col_0")
    c = lax.axis_index("col_1")
    f = (x * NY + y) * NC + c
    g = x * NC + c
    q = y * NZ + z
    xs = [lax.rem(x + k, NX) for k in range(NX)]
    ys = [lax.rem(y + k, NY) for k in range(NY)]
    zs = [lax.rem(z + k, NZ) for k in range(NZ)]
    other = {"row_0": y, "row_1": z, "col_0": x, "col_1": 1 - c}
    along_z = [(zs[k], {"row_0": y, "row_1": zs[k], "col_0": x, "col_1": c}) for k in (4, 3, 5, 2, 6, 1, 7)]

    def chip(k):
        return {"row_0": ys[NEAR[k % NY]], "row_1": z, "col_0": xs[NEAR[k // NY]]}

    plane = [(k, o, {**chip(k), "col_1": 1 - c if o else c}) for k in range(CHIPS) for o in (0, 1) if k or o]
    same_core = [(k, device) for k, o, device in plane if not o]
    row_group = [
        {"row_0": ys[a], "row_1": zs[b], "col_0": x, "col_1": c}
        for b in (4, 3, 5, 2, 6, 1, 7, 0)
        for a in (2, 1, 3, 0)
        if a or b
    ]
    column_group = [(g + 1 - 2 * c, other)] + [
        (xs[a] * NC + o, {"row_0": y, "row_1": z, "col_0": xs[a], "col_1": o}) for a in (2, 1, 3) for o in range(NC)
    ]

    def send(src, dst, sent, arrived, device):
        pltpu.make_async_remote_copy(
            src_ref=src, dst_ref=dst, send_sem=sent, recv_sem=arrived, device_id=device, device_id_type=MESH
        ).start()

    def settle(ref, sem):
        pltpu.make_async_copy(ref, ref, sem).wait()

    def block_at(o):
        return pl.ds(pl.multiple_of(o * BLK, BLK), BLK)

    loads = [
        pltpu.make_async_copy(points_ref, px, sem_in.at[0]),
        pltpu.make_async_copy(ritz_ref, vf.at[0, 0, pl.ds(0, RITZ)], sem_in.at[1]),
        pltpu.make_async_copy(initial_ref, vf.at[0, 0, pl.ds(RITZ, RHS)], sem_in.at[2]),
        pltpu.make_async_copy(targets_ref, tgt, sem_in.at[3]),
        pltpu.make_async_copy(ritz_ref, wz.at[:, block_at(z)], sem_in.at[4]),
    ]
    for load in loads:
        load.start()
    barrier = pltpu.get_barrier_semaphore()
    for device in [d for _, d in along_z] + [d for _, _, d in plane[::-1]]:
        pl.semaphore_signal(barrier, inc=1, device_id=device, device_id_type=MESH)

    gain = gain_ref[0]
    nugget = nugget_ref[0]
    row = lax.broadcasted_iota(jnp.int32, (FEAT, BLK), 0)
    scale = jnp.zeros((FEAT, BLK), F32)
    for i in range(FEAT):
        scale = jnp.where(row == i, scales_ref[i], scale)
    loads[0].wait()
    scaled = px[...] * scale * math.sqrt(LOG2E)
    xf[0, 0] = scaled
    xz[z] = scaled
    for load in loads[1:]:
        load.wait()
    pl.semaphore_wait(barrier, NF - 1 + NZ - 1)

    for _, device in along_z:
        send(xz.at[z], xz.at[z], sxz, rxz, device)
    for k, device in same_core:
        send(xf.at[0, 0], xf.at[0, k], sx, rx, device)
    own_vec = vf.at[0, 0]
    own_w = wz.at[:, block_at(z)]

    def bulk():
        for k, device in same_core:
            send(own_vec, vf.at[0, k], sv, rv, device)
        for _, device in along_z:
            send(own_w, own_w, sw, rw, device)

    if not HOLD:
        bulk()
    settle(xf.at[0, pl.ds(0, CHIPS - 1)], rx)
    send(xf.at[0], xf.at[1], sxf, rxf, other)
    if HOLD:
        bulk()

    def side(h):
        for k in range(CHIPS):
            at = (h * CHIPS + k) * BLK
            ljt[at : at + BLK, :] = features(xf[h, k], True).T.astype(BF16)

    def tile_rows(h):
        @pl.loop(h * HALF // ROWS, (h + 1) * HALF // ROWS)
        def _(i):
            at = pl.ds(pl.multiple_of(i * ROWS, ROWS), ROWS)
            tile = jnp.exp2(jnp.minimum(fast(ljt[at, :], riz[...]), 0.0))
            high = tile.astype(BF16)
            khi[at, :] = high
            klo[at, :] = (tile - high.astype(F32)).astype(BF16)

    side(0)
    settle(xz.at[pl.ds(0, NZ - 1)], rxz)
    for o in range(NZ):
        riz[:, o * BLK : (o + 1) * BLK] = features(xz[o], False).astype(BF16)
    tile_rows(0)
    settle(xf.at[1], rxf)
    side(1)
    tile_rows(1)

    def vectors(h):
        for k in range(CHIPS):
            v = jnp.concatenate([vf[h, k], jnp.zeros((PAD - VEC, BLK), F32)], axis=0)
            at = (h * CHIPS + k) * BLK
            vcat[:, at : at + BLK] = jnp.concatenate(split3(v), axis=0).astype(BF16)

    def product(h):
        at = pl.ds(h * HALF, HALF)

        @pl.loop(0, NI // (2 * BLK))
        def _(p):
            to = pl.ds(pl.multiple_of(p * 2 * BLK, 2 * BLK), 2 * BLK)
            a = fast(vcat[:, at], khi[at, to])
            b = fast(vcat[0 : 2 * PAD, at], klo[at, to])
            total = a[0:VEC] + a[PAD : PAD + VEC] + a[2 * PAD : 2 * PAD + VEC] + b[0:VEC] + b[PAD : PAD + VEC]
            part[:, to] = total if h == 0 else (part[:, to] + total) * gain

    settle(vf.at[0, pl.ds(0, CHIPS - 1)], rv)
    send(vf.at[0], vf.at[1], svf, rvf, other)
    vectors(0)
    product(0)
    settle(vf.at[1], rvf)
    vectors(1)
    product(1)

    mine = part[:, block_at(z)] + nugget * own_vec[...]
    part[:, block_at(z)] = mine
    pin[z] = mine

    lane = lax.broadcasted_iota(jnp.int32, (RITZ, BLK), 1)
    settle(wz.at[:, pl.ds(0, (NZ - 1) * BLK)], rw)
    fill = jnp.zeros((BLK - VEC, NI), F32)
    coarse_part = matmul(wz[...], jnp.concatenate([part[...], fill], axis=0), ((1,), (1,)))
    ritz_own = own_vec[0:RITZ, :]
    start_own = own_vec[RITZ:VEC, :]
    target_rows = jnp.concatenate([jnp.zeros((RITZ, BLK), F32), tgt[...], jnp.zeros((BLK - VEC, BLK), F32)], axis=0)
    coarse_part = jnp.where(lane < RITZ, coarse_part, -coarse_part) + matmul(ritz_own, target_rows, ((1,), (1,)))
    ars[...] = coarse_part.reshape(NG, RHS, BLK)
    for o, device in column_group:
        send(ars.at[o], ara.at[g], sa, ra, device)
    ara[g] = ars[g]
    settle(ara.at[pl.ds(0, NG - 1)], ra)
    arb[q] = jnp.sum(ara[...], axis=0)
    for device in row_group:
        send(arb.at[q], arb.at[q], sb, rb, device)
    for o, device in along_z:
        send(part.at[:, block_at(o)], pin.at[z], sp, rp, device)
    settle(arb.at[pl.ds(0, NQ - 1)], rb)
    arc[g] = jnp.sum(arb[...], axis=0)
    for _, device in column_group:
        send(arc.at[g], arc.at[g], sc, rc, device)
    settle(arc.at[pl.ds(0, NG - 1)], rc)
    first_sum = arc[...].reshape(RITZ, BLK)
    square = jnp.concatenate([first_sum, jnp.zeros((BLK - RITZ, BLK), F32)], axis=0)
    coarse = 0.5 * (first_sum + square.T[0:RITZ])
    sub = lax.broadcasted_iota(jnp.int32, (RITZ, BLK), 0)
    work = jnp.where(lane < RITZ, jnp.where(lane == sub, 1.0, 0.0), pltpu.roll(coarse, RITZ, 1))
    work = eliminate(work)
    inverse = work[:, 0:RITZ]
    amounts = matmul(inverse, first_sum, ((1,), (0,)))
    settle(pin.at[pl.ds(0, NZ - 1)], rp)
    image = jnp.sum(pin[...], axis=0)
    zimg = image[0:RITZ]
    r0 = tgt[...] - image[RITZ:VEC]
    wide = jnp.concatenate([ritz_own, zimg], axis=1)
    moved = matmul(amounts, wide, ((0,), (0,)))[RITZ:VEC]
    resid = r0 - moved[:, BLK:]
    rf[0, 0] = resid
    rz[z] = resid

    for k, o, device in plane[::-1]:
        send(rf.at[0, 0], rf.at[o, k], sr, rr.at[o], device)
    for _, device in along_z:
        send(rz.at[z], rz.at[z], srz, rrz, device)
    sol = start_own + moved[:, 0:BLK]
    lanes = lax.broadcasted_iota(jnp.int32, (RHS, BLK), 1)
    tall = jnp.concatenate([zimg, jnp.zeros((BLK - RITZ, BLK), F32)], axis=0)
    against = matmul(resid, tall, ((1,), (1,)))
    norm = jnp.sum(resid * resid, axis=1, keepdims=True)
    tz[z] = jnp.where(lanes < RITZ, against, jnp.where(lanes == RITZ, norm, 0.0))
    for _, device in along_z:
        send(tz.at[z], tz.at[z], stz, rtz, device)

    def second(h):
        h_, m, low = split3(jnp.concatenate([rf[h, k] for k in range(CHIPS)], axis=1))
        v = jnp.concatenate([h_, m, low, jnp.zeros_like(h_)], axis=0).astype(BF16)
        at = pl.ds(h * HALF, HALF)
        a = fast(v, khi[at, :])
        b = fast(v[0:16], klo[at, :])
        return a[0:8] + a[8:16] + a[16:24] + b[0:8] + b[8:16]

    settle(rf.at[0, pl.ds(0, CHIPS - 1)], rr.at[0])
    acc[...] = second(0)
    settle(rf.at[1], rr.at[1])
    acc[...] = (acc[...] + second(1)) * gain
    settle(rz.at[pl.ds(0, NZ - 1)], rrz)
    acc[:, block_at(z)] = acc[:, block_at(z)] + nugget * resid
    curve = jnp.zeros((RHS, BLK), F32)
    for o in range(NZ):
        curve = curve + acc[:, o * BLK : (o + 1) * BLK] * rz[o]
    for o in range(NZ):
        fs[o, 0:RHS] = acc[:, o * BLK : (o + 1) * BLK]
        fs[o, RHS:] = curve
    for o, device in along_z:
        send(fs.at[o], fr.at[z], ss, rs, device)
    fr[z] = fs[z]
    settle(tz.at[pl.ds(0, NZ - 1)], rtz)
    tf[f] = jnp.sum(tz[...], axis=0)
    for _, _, device in plane[::-1]:
        send(tf.at[f], tf.at[f], st, rt, device)
    settle(fr.at[pl.ds(0, NZ - 1)], rs)
    arrived = jnp.sum(fr[...], axis=0)
    applied, curve = arrived[0:RHS], arrived[RHS:]
    gf[f] = curve
    for _, _, device in plane[::-1]:
        send(gf.at[f], gf.at[f], sg, rg, device)
    settle(tf.at[pl.ds(0, NF - 1)], rt)
    stats = jnp.sum(tf[...], axis=0)
    beta = matmul(stats[:, 0:RITZ], inverse, ((1,), (0,)))
    shift = matmul(beta, wide, ((1,), (0,)))
    direction = resid - shift[:, 0:BLK]
    applied = applied - shift[:, BLK:]
    deflated = jnp.sum(stats[:, 0:RITZ] * beta, axis=1, keepdims=True)
    settle(gf.at[pl.ds(0, NF - 1)], rg)
    curve = jnp.sum(jnp.sum(gf[...], axis=0), axis=1, keepdims=True) - deflated
    step = stats[:, RITZ : RITZ + 1] / curve
    out_ref[...] = sol + step * direction
    res_ref[...] = resid - step * applied

    settle(xf.at[0, pl.ds(0, CHIPS - 1)], sx)
    settle(xf.at[0], sxf)
    settle(xz.at[pl.ds(0, NZ - 1)], sxz)
    settle(vf.at[0, pl.ds(0, CHIPS - 1)], sv)
    settle(vf.at[0], svf)
    settle(wz.at[:, pl.ds(0, (NZ - 1) * BLK)], sw)
    settle(pin.at[pl.ds(0, NZ - 1)], sp)
    settle(ara.at[pl.ds(0, NG - 1)], sa)
    settle(arb.at[pl.ds(0, NQ - 1)], sb)
    settle(arc.at[pl.ds(0, NG - 1)], sc)
    settle(rf.at[0, pl.ds(0, CHIPS - 1)], sr)
    settle(rf.at[1], sr)
    settle(rz.at[pl.ds(0, NZ - 1)], srz)
    settle(tz.at[pl.ds(0, NZ - 1)], stz)
    settle(tf.at[pl.ds(0, NF - 1)], st)
    settle(fr.at[pl.ds(0, NZ - 1)], ss)
    settle(gf.at[pl.ds(0, NF - 1)], sg)


def local(points, inv_scales, amplitude, noise_var, targets, initial, ritz_basis):
    dma = pltpu.SemaphoreType.DMA
    smem = pl.BlockSpec(memory_space=pltpu.SMEM)
    hbm = pl.BlockSpec(memory_space=pl.ANY)
    vmem = pl.BlockSpec(memory_space=pltpu.VMEM)
    return pl.pallas_call(
        body,
        out_shape=(jax.ShapeDtypeStruct((RHS, BLK), F32), jax.ShapeDtypeStruct((RHS, BLK), F32)),
        in_specs=[smem, smem, smem, hbm, hbm, hbm, hbm],
        out_specs=(vmem, vmem),
        scratch_shapes=[
            pltpu.VMEM((FEAT, BLK), F32),
            pltpu.VMEM((NC, CHIPS, FEAT, BLK), F32),
            pltpu.VMEM((NZ, FEAT, BLK), F32),
            pltpu.VMEM((NC, CHIPS, VEC, BLK), F32),
            pltpu.VMEM((RITZ, NI), F32),
            pltpu.VMEM((RHS, BLK), F32),
            pltpu.VMEM((NJ, BLK), BF16),
            pltpu.VMEM((BLK, NI), BF16),
            pltpu.VMEM((NJ, NI), BF16),
            pltpu.VMEM((NJ, NI), BF16),
            pltpu.VMEM((3 * PAD, NJ), BF16),
            pltpu.VMEM((VEC, NI), F32),
            pltpu.VMEM((NZ, VEC, BLK), F32),
            pltpu.VMEM((NG, RHS, BLK), F32),
            pltpu.VMEM((NG, RHS, BLK), F32),
            pltpu.VMEM((NQ, RHS, BLK), F32),
            pltpu.VMEM((NG, RHS, BLK), F32),
            pltpu.VMEM((NC, CHIPS, RHS, BLK), F32),
            pltpu.VMEM((NZ, RHS, BLK), F32),
            pltpu.VMEM((NZ, RHS, BLK), F32),
            pltpu.VMEM((NF, RHS, BLK), F32),
            pltpu.VMEM((RHS, NI), F32),
            pltpu.VMEM((NZ, 2 * RHS, BLK), F32),
            pltpu.VMEM((NZ, 2 * RHS, BLK), F32),
            pltpu.VMEM((NF, RHS, BLK), F32),
            dma((5,)), dma, dma, dma, dma, dma, dma, dma, dma, dma, dma, dma((NC,)), dma, dma, dma, dma, dma,
            dma, dma, dma, dma, dma, dma, dma, dma, dma, dma, dma, dma, dma, dma, dma, dma,
        ],
        compiler_params=pltpu.CompilerParams(
            collective_id=0, has_side_effects=True, vmem_limit_bytes=60 * 1024 * 1024
        ),
    )(amplitude, noise_var, inv_scales, points, targets, initial, ritz_basis)


def solution(mesh):
    torus = Mesh(mesh.devices.reshape(NY, NZ, NX, NC), ("row_0", "row_1", "col_0", "col_1"))
    split = P(None, ("col_0", "col_1", "row_0", "row_1"))
    return jax.shard_map(
        local,
        mesh=torus,
        in_specs=(split, P(), P(), P(), split, split, split),
        out_specs=(split, split),
        check_vma=False,
    )
```

```python
import functools
import math

import jax
import jax.numpy as jnp
from jax import lax
from jax.experimental import pallas as pl
from jax.experimental.pallas import tpu as pltpu
from jax.sharding import Mesh
from jax.sharding import PartitionSpec as P

F32 = jnp.float32
BF16 = jnp.bfloat16
HIGH = lax.Precision.HIGHEST
MESH = pl.DeviceIdType.MESH
NY, NZ, NX, NC = 4, 8, 4, 2
CHIPS = NX * NY
NF = CHIPS * NC
BLK = 128
FEAT = 16
RITZ = 64
RHS = 8
VEC = RITZ + RHS
PAD = 80
NJ = NF * BLK
HALF = CHIPS * BLK
ROWS = 1024
NI = NZ * BLK
NEAR = sorted(((a, b) for a in range(NX) for b in range(NY)), key=lambda o: (min(o[0], NX - o[0]) + min(o[1], NY - o[1]), o))
HERE = CHIPS // 2
FAR = (4, 3, 5, 2, 6, 1, 7, 0)
OWN = NZ - 1
LOG2E = 1.4426950408889634


def split3(a):
    high = a.astype(BF16).astype(F32)
    rest = a - high
    mid = rest.astype(BF16).astype(F32)
    low = (rest - mid).astype(BF16).astype(F32)
    return high, mid, low


def matmul(a, b, dims):
    return lax.dot_general(a, b, (dims, ((), ())), precision=HIGH, preferred_element_type=F32)


def fast(a, b):
    return jnp.dot(a, b, preferred_element_type=F32)


def features(y, left):
    h, m, low = split3(y)
    sh, sm, sl = split3(-0.5 * jnp.sum(y * y, axis=0, keepdims=True))
    row = lax.broadcasted_iota(jnp.int32, (FEAT, BLK), 0)
    at = 0 if left else 3
    ones = (row < 6) & ((row >= 3) if left else (row < 3))
    extra = jnp.where(row == at, sh, jnp.where(row == at + 1, sm, jnp.where(row == at + 2, sl, 0.0)))
    extra = jnp.where(ones, 1.0, extra)
    zero = jnp.zeros((FEAT, BLK), F32)
    parts = [h, m, h, low, h, m, extra, zero] if left else [h, h, m, h, low, m, extra, zero]
    return jnp.concatenate(parts, axis=0)


def inverse2(m):
    a, b, e, d = m
    r = 1.0 / (a * d - b * e)
    return d * r, -b * r, -e * r, a * r


def multiply2(m, n):
    return (
        m[0] * n[0] + m[1] * n[2],
        m[0] * n[1] + m[1] * n[3],
        m[2] * n[0] + m[3] * n[2],
        m[2] * n[1] + m[3] * n[3],
    )


def eliminate(work):
    def full(a):
        return jnp.broadcast_to(a, (RHS, BLK))

    sub = lax.broadcasted_iota(jnp.int32, (RHS, BLK), 0)
    tiles = [work[RHS * i : RHS * (i + 1)] for i in range(RITZ // RHS)]
    for k in range(0, RITZ, 4):
        v, r = k // RHS, k % RHS
        cols = [[full(t[:, RITZ + k + j : RITZ + k + j + 1]) for t in tiles] for j in range(4)]
        u = [full(tiles[v][r + i : r + i + 1]) for i in range(4)]
        m = [[full(cols[j][v][r + i : r + i + 1]) for j in range(4)] for i in range(4)]
        b = (m[0][2], m[0][3], m[1][2], m[1][3])
        first = inverse2((m[0][0], m[0][1], m[1][0], m[1][1]))
        low = multiply2((m[2][0], m[2][1], m[3][0], m[3][1]), first)
        schur = tuple(p - q for p, q in zip((m[2][2], m[2][3], m[3][2], m[3][3]), multiply2(low, b)))
        second = inverse2(schur)
        t2 = u[2] - low[0] * u[0] - low[1] * u[1]
        t3 = u[3] - low[2] * u[0] - low[3] * u[1]
        n2 = second[0] * t2 + second[1] * t3
        n3 = second[2] * t2 + second[3] * t3
        t0 = u[0] - b[0] * n2 - b[1] * n3
        t1 = u[1] - b[2] * n2 - b[3] * n3
        n0 = first[0] * t0 + first[1] * t1
        n1 = first[2] * t0 + first[3] * t1
        for j in range(4):
            cols[j][v] = jnp.where(sub == r + j, cols[j][v] - 1.0, cols[j][v])
        tiles = [
            t - (cols[0][i] * n0 + cols[1][i] * n1) - (cols[2][i] * n2 + cols[3][i] * n3)
            for i, t in enumerate(tiles)
        ]
    return jnp.concatenate(tiles, axis=0)


def body(
    gain_ref, nugget_ref, scales_ref, points_ref, targets_ref, initial_ref, ritz_ref, out_ref,
    gain_at, nugget_at, scales_at, px, xf, xz, vf, wz, tgt, ljt, riz, khi, klo, vcat, part, pin, ars, ara, arb, arc, rf, rz, tz, tf, acc, fr, gf, hz,
    sem_in, rx, rxf, rxz, rv, rvf, rw, rp, ra, rb, rc, rr, rrz, rtz, rt, rs, rg, rh,
    sx, sxf, sxz, sv, svf, sw, sp, sa, sb, sc, sr, srz, stz, st, ss, sg, sh,
):
    y = lax.axis_index("row_0")
    z = lax.axis_index("row_1")
    x = lax.axis_index("col_0")
    c = lax.axis_index("col_1")
    f = (x * NY + y) * NC + c
    xs = [lax.rem(x + k, NX) for k in range(NX)]
    ys = [lax.rem(y + k, NY) for k in range(NY)]
    zs = [lax.rem(z + k, NZ) for k in range(NZ)]
    other = {"row_0": y, "row_1": z, "col_0": x, "col_1": 1 - c}
    along_z = [
        (FAR.index((NZ - k) % NZ), i, {"row_0": y, "row_1": zs[k], "col_0": x, "col_1": c}) for i, k in enumerate(FAR[:-1])
    ]

    def chip(k):
        return {"row_0": ys[NEAR[k][1]], "row_1": z, "col_0": xs[NEAR[k][0]]}

    plane = [(k, o, {**chip(k), "col_1": 1 - c if o else c}) for k in range(CHIPS) for o in (0, 1) if k or o]
    same_core = [(k, device) for k, o, device in plane if not o]
    def send(src, dst, sent, arrived, device):
        pltpu.make_async_remote_copy(
            src_ref=src, dst_ref=dst, send_sem=sent, recv_sem=arrived, device_id=device, device_id_type=MESH
        ).start()

    def settle(ref, sem):
        pltpu.make_async_copy(ref, ref, sem).wait()

    loads = [
        pltpu.make_async_copy(scales_ref, scales_at, sem_in.at[5]),
        pltpu.make_async_copy(gain_ref, gain_at, sem_in.at[6]),
        pltpu.make_async_copy(nugget_ref, nugget_at, sem_in.at[7]),
        pltpu.make_async_copy(points_ref, px, sem_in.at[0]),
        pltpu.make_async_copy(ritz_ref, vf.at[0, 0, pl.ds(0, RITZ)], sem_in.at[1]),
        pltpu.make_async_copy(initial_ref, vf.at[0, 0, pl.ds(RITZ, RHS)], sem_in.at[2]),
        pltpu.make_async_copy(targets_ref, tgt, sem_in.at[3]),
        pltpu.make_async_copy(ritz_ref, wz.at[:, OWN * BLK :], sem_in.at[4]),
    ]
    for load in loads:
        load.start()
    barrier = pltpu.get_barrier_semaphore()
    for device in [d for _, _, d in along_z] + [d for _, _, d in plane[::-1]]:
        pl.semaphore_signal(barrier, inc=1, device_id=device, device_id_type=MESH)

    row = lax.broadcasted_iota(jnp.int32, (FEAT, BLK), 0)
    for load in loads[:4]:
        load.wait()
    gain = gain_at[0]
    nugget = nugget_at[0]
    scale = jnp.zeros((FEAT, BLK), F32)
    for i in range(FEAT):
        scale = jnp.where(row == i, scales_at[i], scale)
    scaled = px[...] * scale * math.sqrt(LOG2E)
    xf[0, 0] = scaled
    xz[OWN] = scaled
    for load in loads[4:]:
        load.wait()
    pl.semaphore_wait(barrier, NF - 1 + NZ - 1)

    for there, _, device in along_z:
        send(xz.at[OWN], xz.at[there], sxz, rxz, device)
    for k, device in same_core:
        send(xf.at[0, 0], xf.at[0, k], sx, rx, device)
    own_vec = vf.at[0, 0]
    own_w = wz.at[:, OWN * BLK :]

    def bulk():
        for k, device in same_core:
            send(own_vec, vf.at[0, k], sv, rv.at[k // HERE], device)
        for there, _, device in along_z:
            send(own_w, wz.at[:, there * BLK : (there + 1) * BLK], sw, rw, device)

    bulk()
    settle(xf.at[0, pl.ds(0, CHIPS - 1)], rx)
    send(xf.at[0], xf.at[1], sxf, rxf, other)

    def side(h):
        for k in range(CHIPS):
            at = (h * CHIPS + k) * BLK
            ljt[at : at + BLK, :] = features(xf[h, k], True).T.astype(BF16)

    def tile_rows(i):
        at = pl.ds(i * ROWS, ROWS)
        tile = jnp.exp2(jnp.minimum(fast(ljt[at, :], riz[...]), 0.0))
        high = tile.astype(BF16)
        khi[at, :] = high
        klo[at, :] = (tile - high.astype(F32)).astype(BF16)

    side(0)
    settle(xz.at[pl.ds(0, NZ - 1)], rxz)
    for o in range(NZ):
        riz[:, o * BLK : (o + 1) * BLK] = features(xz[o], False).astype(BF16)
    tile_rows(0)
    tile_rows(1)
    settle(xf.at[1], rxf)
    side(1)
    tile_rows(2)
    settle(vf.at[0, pl.ds(1, HERE - 1)], rv.at[0])
    send(vf.at[0, pl.ds(0, HERE)], vf.at[1, pl.ds(0, HERE)], svf.at[0], rvf.at[0], other)
    tile_rows(3)

    def vectors(h, near):
        for k in range(0 if near else HERE, HERE if near else CHIPS):
            high, mid, low = split3(vf[h, k])
            at = (h * CHIPS + k) * BLK
            v = jnp.concatenate([high, low[RITZ:], mid, jnp.zeros((PAD - VEC, BLK), F32)], axis=0)
            vcat[:, at : at + BLK] = v.astype(BF16)

    def product(h, near):
        vectors(h, near)
        at = pl.ds((h * CHIPS + (0 if near else HERE)) * BLK, HERE * BLK)
        a = fast(vcat[:, at], khi[at, :])
        b = fast(vcat[0:PAD, at], klo[at, :])
        low = jnp.concatenate([jnp.zeros((RITZ, NI), F32), a[VEC:PAD] + b[VEC:PAD]], axis=0)
        return a[0:VEC] + a[PAD : PAD + VEC] + b[0:VEC] + low

    part[...] = product(0, True)
    settle(vf.at[1, pl.ds(0, HERE)], rvf.at[0])
    part[...] = part[...] + product(1, True)
    settle(vf.at[0, pl.ds(HERE, HERE)], rv.at[1])
    send(vf.at[0, pl.ds(HERE, HERE)], vf.at[1, pl.ds(HERE, HERE)], svf.at[1], rvf.at[1], other)
    part[...] = part[...] + product(0, False)
    settle(vf.at[1, pl.ds(HERE, HERE)], rvf.at[1])
    part[...] = (part[...] + product(1, False)) * gain

    mine = part[:, OWN * BLK :] + nugget * own_vec[...]
    part[:, OWN * BLK :] = mine
    pin[z] = mine

    lane = lax.broadcasted_iota(jnp.int32, (RITZ, BLK), 1)
    settle(wz.at[:, pl.ds(0, (NZ - 1) * BLK)], rw)
    fill = jnp.zeros((BLK - VEC, NI), F32)
    coarse_part = matmul(wz[...], jnp.concatenate([part[...], fill], axis=0), ((1,), (1,)))
    ritz_own = own_vec[0:RITZ, :]
    start_own = own_vec[RITZ:VEC, :]
    target_rows = jnp.concatenate([jnp.zeros((RITZ, BLK), F32), tgt[...], jnp.zeros((BLK - VEC, BLK), F32)], axis=0)
    coarse_part = jnp.where(lane < RITZ, coarse_part, -coarse_part) + matmul(ritz_own, target_rows, ((1,), (1,)))
    ars[...] = coarse_part.reshape(NZ, RHS, BLK)
    for _, here, device in along_z:
        send(ars.at[zs[FAR[here]]], ara.at[z], sa, ra, device)
    for _, here, device in along_z:
        send(part.at[:, here * BLK : (here + 1) * BLK], pin.at[z], sp, rp, device)
    ara[z] = ars[z]
    settle(ara.at[pl.ds(0, NZ - 1)], ra)
    arb[f] = jnp.sum(ara[...], axis=0)
    for _, _, device in plane[::-1]:
        send(arb.at[f], arb.at[f], sb, rb, device)
    settle(arb.at[pl.ds(0, NF - 1)], rb)
    arc[z] = jnp.sum(arb[...], axis=0)
    for _, _, device in along_z:
        send(arc.at[z], arc.at[z], sc, rc, device)
    settle(arc.at[pl.ds(0, NZ - 1)], rc)
    first_sum = arc[...].reshape(RITZ, BLK)
    square = jnp.concatenate([first_sum, jnp.zeros((BLK - RITZ, BLK), F32)], axis=0)
    coarse = 0.5 * (first_sum + square.T[0:RITZ])
    sub = lax.broadcasted_iota(jnp.int32, (RITZ, BLK), 0)
    work = jnp.where(lane < RITZ, jnp.where(lane == sub, 1.0, 0.0), pltpu.roll(coarse, RITZ, 1))
    work = eliminate(work)
    inverse = work[:, 0:RITZ]
    amounts = matmul(inverse, first_sum, ((1,), (0,)))
    settle(pin.at[pl.ds(0, NZ - 1)], rp)
    image = jnp.sum(pin[...], axis=0)
    zimg = image[0:RITZ]
    r0 = tgt[...] - image[RITZ:VEC]
    wide = jnp.concatenate([ritz_own, zimg], axis=1)
    moved = matmul(amounts, wide, ((0,), (0,)))[RITZ:VEC]
    resid = r0 - moved[:, BLK:]
    rf[0, 0] = resid
    rz[OWN] = resid

    for k, o, device in plane[::-1]:
        send(rf.at[0, 0], rf.at[o, k], sr, rr.at[k // HERE], device)
    for there, _, device in along_z:
        send(rz.at[OWN], rz.at[there], srz, rrz, device)
    sol = start_own + moved[:, 0:BLK]
    lanes = lax.broadcasted_iota(jnp.int32, (RHS, BLK), 1)
    tall = jnp.concatenate([zimg, jnp.zeros((BLK - RITZ, BLK), F32)], axis=0)
    against = matmul(resid, tall, ((1,), (1,)))
    norm = jnp.sum(resid * resid, axis=1, keepdims=True)
    tz[z] = jnp.where(lanes < RITZ, against, jnp.where(lanes == RITZ, norm, 0.0))
    for _, _, device in along_z:
        send(tz.at[z], tz.at[z], stz, rtz, device)

    def second(near):
        total = None
        for h in range(NC):
            slots = range(0 if near else HERE, HERE if near else CHIPS)
            high, mid, low = split3(jnp.concatenate([rf[h, k] for k in slots], axis=1))
            v = jnp.concatenate([high, mid, low, jnp.zeros_like(high)], axis=0).astype(BF16)
            at = pl.ds((h * CHIPS + slots[0]) * BLK, HERE * BLK)
            a = fast(v, khi[at, :])
            b = fast(v[0:16], klo[at, :])
            one = a[0:8] + a[8:16] + a[16:24] + b[0:8] + b[8:16]
            total = one if total is None else total + one
        return total

    settle(rf.at[0, pl.ds(0, 2 * HERE - 1)], rr.at[0])
    acc[...] = second(True)
    settle(tz.at[pl.ds(0, NZ - 1)], rtz)
    tf[f] = jnp.sum(tz[...], axis=0)
    for _, _, device in plane[::-1]:
        send(tf.at[f], tf.at[f], st, rt, device)
    settle(rf.at[:, pl.ds(HERE, HERE)], rr.at[1])
    acc[...] = (acc[...] + second(False)) * gain
    settle(rz.at[pl.ds(0, NZ - 1)], rrz)
    acc[:, OWN * BLK :] = acc[:, OWN * BLK :] + nugget * resid
    curve = jnp.zeros((RHS, BLK), F32)
    for o in range(NZ):
        curve = curve + acc[:, o * BLK : (o + 1) * BLK] * rz[o]
    curve = jnp.sum(curve, axis=1, keepdims=True)
    here_lane = lanes == lax.broadcasted_iota(jnp.int32, (RHS, BLK), 0)
    gf[f] = jnp.sum(jnp.where(here_lane, curve, 0.0), axis=0, keepdims=True)
    for _, _, device in plane[::-1]:
        send(gf.at[f], gf.at[f], sg, rg, device)
    for _, here, device in along_z:
        send(acc.at[:, here * BLK : (here + 1) * BLK], fr.at[z], ss, rs, device)
    fr[z] = acc[:, OWN * BLK :]
    settle(gf.at[pl.ds(0, NF - 1)], rg)
    hz[z] = jnp.sum(gf[...], axis=0)
    for _, _, device in along_z:
        send(hz.at[z], hz.at[z], sh, rh, device)
    settle(tf.at[pl.ds(0, NF - 1)], rt)
    stats = jnp.sum(tf[...], axis=0)
    beta = matmul(stats[:, 0:RITZ], inverse, ((1,), (0,)))
    shift = matmul(beta, wide, ((1,), (0,)))
    direction = resid - shift[:, 0:BLK]
    deflated = jnp.sum(stats[:, 0:RITZ] * beta, axis=1, keepdims=True)
    settle(fr.at[pl.ds(0, NZ - 1)], rs)
    applied = jnp.sum(fr[...], axis=0) - shift[:, BLK:]
    settle(hz.at[pl.ds(0, NZ - 1)], rh)
    curve = jnp.sum(jnp.where(here_lane, jnp.sum(hz[...], axis=0), 0.0), axis=1, keepdims=True) - deflated
    step = stats[:, RITZ : RITZ + 1] / curve
    out_ref[0:RHS] = sol + step * direction
    out_ref[RHS:] = resid - step * applied

    settle(xf.at[0, pl.ds(0, CHIPS - 1)], sx)
    settle(xf.at[0], sxf)
    settle(xz.at[pl.ds(0, NZ - 1)], sxz)
    settle(vf.at[0, pl.ds(0, CHIPS - 1)], sv)
    for o in range(2):
        settle(vf.at[0, pl.ds(0, HERE)], svf.at[o])
    settle(wz.at[:, pl.ds(0, (NZ - 1) * BLK)], sw)
    settle(pin.at[pl.ds(0, NZ - 1)], sp)
    settle(ara.at[pl.ds(0, NZ - 1)], sa)
    settle(arb.at[pl.ds(0, NF - 1)], sb)
    settle(arc.at[pl.ds(0, NZ - 1)], sc)
    settle(rf.at[0, pl.ds(0, CHIPS - 1)], sr)
    settle(rf.at[1], sr)
    settle(rz.at[pl.ds(0, NZ - 1)], srz)
    settle(tz.at[pl.ds(0, NZ - 1)], stz)
    settle(fr.at[pl.ds(0, NZ - 1)], ss)
    settle(tf.at[pl.ds(0, NF - 1)], st)
    settle(gf.at[pl.ds(0, NF - 1)], sg)
    settle(hz.at[pl.ds(0, NZ - 1)], sh)


def local(points, inv_scales, amplitude, noise_var, targets, initial, ritz_basis):
    dma = pltpu.SemaphoreType.DMA
    hbm = pl.BlockSpec(memory_space=pltpu.HBM)
    vmem = pl.BlockSpec(memory_space=pltpu.VMEM)
    both = pl.pallas_call(
        body,
        out_shape=pltpu.VMEM((2 * RHS, BLK), F32),
        in_specs=[hbm, hbm, hbm, hbm, hbm, hbm, hbm],
        out_specs=vmem,
        scratch_shapes=[
            pltpu.SMEM((1,), F32),
            pltpu.SMEM((1,), F32),
            pltpu.SMEM((FEAT,), F32),
            pltpu.VMEM((FEAT, BLK), F32),
            pltpu.VMEM((NC, CHIPS, FEAT, BLK), F32),
            pltpu.VMEM((NZ, FEAT, BLK), F32),
            pltpu.VMEM((NC, CHIPS, VEC, BLK), F32),
            pltpu.VMEM((RITZ, NI), F32),
            pltpu.VMEM((RHS, BLK), F32),
            pltpu.VMEM((NJ, BLK), BF16),
            pltpu.VMEM((BLK, NI), BF16),
            pltpu.VMEM((NJ, NI), BF16),
            pltpu.VMEM((NJ, NI), BF16),
            pltpu.VMEM((2 * PAD, NJ), BF16),
            pltpu.VMEM((VEC, NI), F32),
            pltpu.VMEM((NZ, VEC, BLK), F32),
            pltpu.VMEM((NZ, RHS, BLK), F32),
            pltpu.VMEM((NZ, RHS, BLK), F32),
            pltpu.VMEM((NF, RHS, BLK), F32),
            pltpu.VMEM((NZ, RHS, BLK), F32),
            pltpu.VMEM((NC, CHIPS, RHS, BLK), F32),
            pltpu.VMEM((NZ, RHS, BLK), F32),
            pltpu.VMEM((NZ, RHS, BLK), F32),
            pltpu.VMEM((NF, RHS, BLK), F32),
            pltpu.VMEM((RHS, NI), F32),
            pltpu.VMEM((NZ, RHS, BLK), F32),
            pltpu.VMEM((NF, 1, BLK), F32),
            pltpu.VMEM((NZ, 1, BLK), F32),
            dma((8,)), dma, dma, dma, dma((2,)), dma((2,)), dma, dma, dma, dma, dma, dma((2,)), dma, dma, dma, dma, dma, dma,
            dma, dma, dma, dma, dma((2,)), dma, dma, dma, dma, dma, dma, dma, dma, dma, dma, dma, dma,
        ],
        compiler_params=pltpu.CompilerParams(
            collective_id=0, has_side_effects=True, vmem_limit_bytes=60 * 1024 * 1024
        ),
    )(amplitude, noise_var, inv_scales, points, targets, initial, ritz_basis)
    return both[:RHS], both[RHS:]


def solution(mesh):
    torus = Mesh(mesh.devices.reshape(NY, NZ, NX, NC), ("row_0", "row_1", "col_0", "col_1"))
    split = P(None, ("col_0", "col_1", "row_0", "row_1"))
    return jax.shard_map(
        local,
        mesh=torus,
        in_specs=(split, P(), P(), P(), split, split, split),
        out_specs=(split, split),
        check_vma=False,
    )
```

```python
import functools
import math

import jax
import jax.numpy as jnp
from jax import lax
from jax.experimental import pallas as pl
from jax.experimental.pallas import tpu as pltpu
from jax.sharding import Mesh
from jax.sharding import PartitionSpec as P

F32 = jnp.float32
BF16 = jnp.bfloat16
HIGH = lax.Precision.HIGHEST
MESH = pl.DeviceIdType.MESH
NY, NZ, NX, NC = 4, 8, 4, 2
CHIPS = NX * NY
NF = CHIPS * NC
BLK = 128
FEAT = 16
RITZ = 64
RHS = 8
VEC = RITZ + RHS
PAD = 80
NJ = NF * BLK
HALF = CHIPS * BLK
ROWS = 1024
NI = NZ * BLK
NEAR = sorted(((a, b) for a in range(NX) for b in range(NY)), key=lambda o: (min(o[0], NX - o[0]) + min(o[1], NY - o[1]), o))
HERE = CHIPS // 2
FAR = (4, 3, 5, 2, 6, 1, 7, 0)
OWN = NZ - 1
LOG2E = 1.4426950408889634


def split3(a):
    high = a.astype(BF16).astype(F32)
    rest = a - high
    mid = rest.astype(BF16).astype(F32)
    low = (rest - mid).astype(BF16).astype(F32)
    return high, mid, low


def matmul(a, b, dims):
    return lax.dot_general(a, b, (dims, ((), ())), precision=HIGH, preferred_element_type=F32)


def fast(a, b):
    return jnp.dot(a, b, preferred_element_type=F32)


def features(y, left):
    h, m, low = split3(y)
    sh, sm, sl = split3(-0.5 * jnp.sum(y * y, axis=0, keepdims=True))
    row = lax.broadcasted_iota(jnp.int32, (FEAT, BLK), 0)
    at = 0 if left else 3
    ones = (row < 6) & ((row >= 3) if left else (row < 3))
    extra = jnp.where(row == at, sh, jnp.where(row == at + 1, sm, jnp.where(row == at + 2, sl, 0.0)))
    extra = jnp.where(ones, 1.0, extra)
    zero = jnp.zeros((FEAT, BLK), F32)
    parts = [h, m, h, low, h, m, extra, zero] if left else [h, h, m, h, low, m, extra, zero]
    return jnp.concatenate(parts, axis=0)


def inverse2(m):
    a, b, e, d = m
    r = 1.0 / (a * d - b * e)
    return d * r, -b * r, -e * r, a * r


def multiply2(m, n):
    return (
        m[0] * n[0] + m[1] * n[2],
        m[0] * n[1] + m[1] * n[3],
        m[2] * n[0] + m[3] * n[2],
        m[2] * n[1] + m[3] * n[3],
    )


def eliminate(work):
    def full(a):
        return jnp.broadcast_to(a, (RHS, BLK))

    sub = lax.broadcasted_iota(jnp.int32, (RHS, BLK), 0)
    tiles = [work[RHS * i : RHS * (i + 1)] for i in range(RITZ // RHS)]
    for k in range(0, RITZ, 4):
        v, r = k // RHS, k % RHS
        cols = [[full(t[:, RITZ + k + j : RITZ + k + j + 1]) for t in tiles] for j in range(4)]
        u = [full(tiles[v][r + i : r + i + 1]) for i in range(4)]
        m = [[full(cols[j][v][r + i : r + i + 1]) for j in range(4)] for i in range(4)]
        b = (m[0][2], m[0][3], m[1][2], m[1][3])
        first = inverse2((m[0][0], m[0][1], m[1][0], m[1][1]))
        low = multiply2((m[2][0], m[2][1], m[3][0], m[3][1]), first)
        schur = tuple(p - q for p, q in zip((m[2][2], m[2][3], m[3][2], m[3][3]), multiply2(low, b)))
        second = inverse2(schur)
        t2 = u[2] - low[0] * u[0] - low[1] * u[1]
        t3 = u[3] - low[2] * u[0] - low[3] * u[1]
        n2 = second[0] * t2 + second[1] * t3
        n3 = second[2] * t2 + second[3] * t3
        t0 = u[0] - b[0] * n2 - b[1] * n3
        t1 = u[1] - b[2] * n2 - b[3] * n3
        n0 = first[0] * t0 + first[1] * t1
        n1 = first[2] * t0 + first[3] * t1
        for j in range(4):
            cols[j][v] = jnp.where(sub == r + j, cols[j][v] - 1.0, cols[j][v])
        tiles = [
            t - (cols[0][i] * n0 + cols[1][i] * n1) - (cols[2][i] * n2 + cols[3][i] * n3)
            for i, t in enumerate(tiles)
        ]
    return jnp.concatenate(tiles, axis=0)


def body(
    gain_ref, nugget_ref, scales_ref, points_ref, targets_ref, initial_ref, ritz_ref, out_ref,
    gain_at, nugget_at, scales_at, px, xf, xz, vf, wz, tgt, ljt, riz, khi, klo, vcat, part, pin, ars, ara, arb, arc, rf, rz, tz, tf, acc, fr, gf, hz,
    sem_in, rx, rxf, rxz, rv, rvf, rw, rp, ra, rb, rc, rr, rrz, rtz, rt, rs, rg, rh,
    sx, sxf, sxz, sv, svf, sw, sp, sa, sb, sc, sr, srz, stz, st, ss, sg, sh,
):
    y = lax.axis_index("row_0")
    z = lax.axis_index("row_1")
    x = lax.axis_index("col_0")
    c = lax.axis_index("col_1")
    f = (x * NY + y) * NC + c
    xs = [lax.rem(x + k, NX) for k in range(NX)]
    ys = [lax.rem(y + k, NY) for k in range(NY)]
    zs = [lax.rem(z + k, NZ) for k in range(NZ)]
    other = {"row_0": y, "row_1": z, "col_0": x, "col_1": 1 - c}
    along_z = [
        (FAR.index((NZ - k) % NZ), i, {"row_0": y, "row_1": zs[k], "col_0": x, "col_1": c}) for i, k in enumerate(FAR[:-1])
    ]

    def chip(k):
        return {"row_0": ys[NEAR[k][1]], "row_1": z, "col_0": xs[NEAR[k][0]]}

    plane = [(k, o, {**chip(k), "col_1": 1 - c if o else c}) for k in range(CHIPS) for o in (0, 1) if k or o]
    same_core = [(k, device) for k, o, device in plane if not o]
    def send(src, dst, sent, arrived, device):
        pltpu.make_async_remote_copy(
            src_ref=src, dst_ref=dst, send_sem=sent, recv_sem=arrived, device_id=device, device_id_type=MESH
        ).start()

    def settle(ref, sem):
        pltpu.make_async_copy(ref, ref, sem).wait()

    loads = [
        pltpu.make_async_copy(scales_ref, scales_at, sem_in.at[5]),
        pltpu.make_async_copy(gain_ref, gain_at, sem_in.at[6]),
        pltpu.make_async_copy(nugget_ref, nugget_at, sem_in.at[7]),
        pltpu.make_async_copy(points_ref, px, sem_in.at[0]),
        pltpu.make_async_copy(ritz_ref, vf.at[0, 0, pl.ds(0, RITZ)], sem_in.at[1]),
        pltpu.make_async_copy(initial_ref, vf.at[0, 0, pl.ds(RITZ, RHS)], sem_in.at[2]),
        pltpu.make_async_copy(targets_ref, tgt, sem_in.at[3]),
        pltpu.make_async_copy(ritz_ref, wz.at[:, OWN * BLK :], sem_in.at[4]),
    ]
    for load in loads:
        load.start()
    barrier = pltpu.get_barrier_semaphore()
    for device in [d for _, _, d in along_z] + [d for _, _, d in plane[::-1]]:
        pl.semaphore_signal(barrier, inc=1, device_id=device, device_id_type=MESH)

    row = lax.broadcasted_iota(jnp.int32, (FEAT, BLK), 0)
    for load in loads[:4]:
        load.wait()
    gain = gain_at[0]
    nugget = nugget_at[0]
    scale = jnp.zeros((FEAT, BLK), F32)
    for i in range(FEAT):
        scale = jnp.where(row == i, scales_at[i], scale)
    scaled = px[...] * scale * math.sqrt(LOG2E)
    xf[0, 0] = scaled
    xz[OWN] = scaled
    for load in loads[4:]:
        load.wait()
    pl.delay(1)
    pl.semaphore_wait(barrier, NF - 1 + NZ - 1)

    pl.delay(1)
    for there, _, device in along_z:
        send(xz.at[OWN], xz.at[there], sxz, rxz, device)
    for k, device in same_core:
        send(xf.at[0, 0], xf.at[0, k], sx, rx, device)
    own_vec = vf.at[0, 0]
    own_w = wz.at[:, OWN * BLK :]

    def bulk():
        for k, device in same_core:
            send(own_vec, vf.at[0, k], sv, rv.at[k // HERE], device)
        for there, _, device in along_z:
            send(own_w, wz.at[:, there * BLK : (there + 1) * BLK], sw, rw, device)

    bulk()
    pl.delay(1)
    settle(xf.at[0, pl.ds(0, CHIPS - 1)], rx)
    send(xf.at[0], xf.at[1], sxf, rxf, other)

    def side(h):
        for k in range(CHIPS):
            at = (h * CHIPS + k) * BLK
            ljt[at : at + BLK, :] = features(xf[h, k], True).T.astype(BF16)

    def tile_rows(i):
        at = pl.ds(i * ROWS, ROWS)
        for to in (pl.ds(0, NI // 2), pl.ds(NI // 2, NI // 2)):
            tile = jnp.exp2(jnp.minimum(fast(ljt[at, :], riz[:, to]), 0.0))
            high = tile.astype(BF16)
            khi[at, to] = high
            klo[at, to] = (tile - high.astype(F32)).astype(BF16)

    pl.delay(1)
    side(0)
    pl.delay(1)
    settle(xz.at[pl.ds(0, NZ - 1)], rxz)
    pl.delay(1)
    for o in range(NZ):
        riz[:, o * BLK : (o + 1) * BLK] = features(xz[o], False).astype(BF16)
    pl.delay(1)
    tile_rows(0)
    tile_rows(1)
    pl.delay(1)
    settle(xf.at[1], rxf)
    pl.delay(1)
    side(1)
    pl.delay(1)
    tile_rows(2)
    pl.delay(1)
    settle(vf.at[0, pl.ds(1, HERE - 1)], rv.at[0])
    send(vf.at[0, pl.ds(0, HERE)], vf.at[1, pl.ds(0, HERE)], svf.at[0], rvf.at[0], other)
    pl.delay(1)
    tile_rows(3)

    def vectors(h, near):
        for k in range(0 if near else HERE, HERE if near else CHIPS):
            high, mid, low = split3(vf[h, k])
            at = (h * CHIPS + k) * BLK
            v = jnp.concatenate([high, low[RITZ:], mid, jnp.zeros((PAD - VEC, BLK), F32)], axis=0)
            vcat[:, at : at + BLK] = v.astype(BF16)

    def product(h, near):
        vectors(h, near)
        at = pl.ds((h * CHIPS + (0 if near else HERE)) * BLK, HERE * BLK)
        a = fast(vcat[:, at], khi[at, :])
        b = fast(vcat[0:PAD, at], klo[at, :])
        low = jnp.concatenate([jnp.zeros((RITZ, NI), F32), a[VEC:PAD] + b[VEC:PAD]], axis=0)
        return a[0:VEC] + a[PAD : PAD + VEC] + b[0:VEC] + low

    pl.delay(1)
    part[...] = product(0, True)
    pl.delay(1)
    settle(vf.at[1, pl.ds(0, HERE)], rvf.at[0])
    pl.delay(1)
    part[...] = part[...] + product(1, True)
    pl.delay(1)
    settle(vf.at[0, pl.ds(HERE, HERE)], rv.at[1])
    send(vf.at[0, pl.ds(HERE, HERE)], vf.at[1, pl.ds(HERE, HERE)], svf.at[1], rvf.at[1], other)
    pl.delay(1)
    part[...] = part[...] + product(0, False)
    pl.delay(1)
    settle(vf.at[1, pl.ds(HERE, HERE)], rvf.at[1])
    pl.delay(1)
    part[...] = (part[...] + product(1, False)) * gain

    pl.delay(1)
    mine = part[:, OWN * BLK :] + nugget * own_vec[...]
    part[:, OWN * BLK :] = mine
    pin[z] = mine

    lane = lax.broadcasted_iota(jnp.int32, (RITZ, BLK), 1)
    pl.delay(1)
    settle(wz.at[:, pl.ds(0, (NZ - 1) * BLK)], rw)
    pl.delay(1)
    fill = jnp.zeros((BLK - VEC, NI), F32)
    coarse_part = matmul(wz[...], jnp.concatenate([part[...], fill], axis=0), ((1,), (1,)))
    ritz_own = own_vec[0:RITZ, :]
    start_own = own_vec[RITZ:VEC, :]
    target_rows = jnp.concatenate([jnp.zeros((RITZ, BLK), F32), tgt[...], jnp.zeros((BLK - VEC, BLK), F32)], axis=0)
    coarse_part = jnp.where(lane < RITZ, coarse_part, -coarse_part) + matmul(ritz_own, target_rows, ((1,), (1,)))
    ars[...] = coarse_part.reshape(NZ, RHS, BLK)
    for _, here, device in along_z:
        send(ars.at[zs[FAR[here]]], ara.at[z], sa, ra, device)
    for _, here, device in along_z:
        send(part.at[:, here * BLK : (here + 1) * BLK], pin.at[z], sp, rp, device)
    ara[z] = ars[z]
    pl.delay(1)
    settle(ara.at[pl.ds(0, NZ - 1)], ra)
    arb[f] = jnp.sum(ara[...], axis=0)
    for _, _, device in plane[::-1]:
        send(arb.at[f], arb.at[f], sb, rb, device)
    pl.delay(1)
    settle(arb.at[pl.ds(0, NF - 1)], rb)
    arc[z] = jnp.sum(arb[...], axis=0)
    for _, _, device in along_z:
        send(arc.at[z], arc.at[z], sc, rc, device)
    pl.delay(1)
    settle(arc.at[pl.ds(0, NZ - 1)], rc)
    pl.delay(1)
    first_sum = arc[...].reshape(RITZ, BLK)
    square = jnp.concatenate([first_sum, jnp.zeros((BLK - RITZ, BLK), F32)], axis=0)
    coarse = 0.5 * (first_sum + square.T[0:RITZ])
    sub = lax.broadcasted_iota(jnp.int32, (RITZ, BLK), 0)
    work = jnp.where(lane < RITZ, jnp.where(lane == sub, 1.0, 0.0), pltpu.roll(coarse, RITZ, 1))
    work = eliminate(work)
    inverse = work[:, 0:RITZ]
    pl.delay(1)
    amounts = matmul(inverse, first_sum, ((1,), (0,)))
    pl.delay(1)
    settle(pin.at[pl.ds(0, NZ - 1)], rp)
    image = jnp.sum(pin[...], axis=0)
    zimg = image[0:RITZ]
    r0 = tgt[...] - image[RITZ:VEC]
    pl.delay(1)
    wide = jnp.concatenate([ritz_own, zimg], axis=1)
    moved = matmul(amounts, wide, ((0,), (0,)))[RITZ:VEC]
    resid = r0 - moved[:, BLK:]
    rf[0, 0] = resid
    rz[OWN] = resid

    pl.delay(1)
    for k, o, device in plane[::-1]:
        send(rf.at[0, 0], rf.at[o, k], sr, rr.at[k // HERE], device)
    for there, _, device in along_z:
        send(rz.at[OWN], rz.at[there], srz, rrz, device)
    pl.delay(1)
    sol = start_own + moved[:, 0:BLK]
    lanes = lax.broadcasted_iota(jnp.int32, (RHS, BLK), 1)
    tall = jnp.concatenate([zimg, jnp.zeros((BLK - RITZ, BLK), F32)], axis=0)
    against = matmul(resid, tall, ((1,), (1,)))
    norm = jnp.sum(resid * resid, axis=1, keepdims=True)
    tz[z] = jnp.where(lanes < RITZ, against, jnp.where(lanes == RITZ, norm, 0.0))
    for _, _, device in along_z:
        send(tz.at[z], tz.at[z], stz, rtz, device)

    def second(near):
        total = None
        for h in range(NC):
            slots = range(0 if near else HERE, HERE if near else CHIPS)
            high, mid, low = split3(jnp.concatenate([rf[h, k] for k in slots], axis=1))
            v = jnp.concatenate([high, mid, low, jnp.zeros_like(high)], axis=0).astype(BF16)
            at = pl.ds((h * CHIPS + slots[0]) * BLK, HERE * BLK)
            a = fast(v, khi[at, :])
            b = fast(v[0:16], klo[at, :])
            one = a[0:8] + a[8:16] + a[16:24] + b[0:8] + b[8:16]
            total = one if total is None else total + one
        return total

    pl.delay(1)
    settle(rf.at[0, pl.ds(0, 2 * HERE - 1)], rr.at[0])
    pl.delay(1)
    acc[...] = second(True)
    settle(tz.at[pl.ds(0, NZ - 1)], rtz)
    tf[f] = jnp.sum(tz[...], axis=0)
    for _, _, device in plane[::-1]:
        send(tf.at[f], tf.at[f], st, rt, device)
    pl.delay(1)
    settle(rf.at[:, pl.ds(HERE, HERE)], rr.at[1])
    pl.delay(1)
    acc[...] = (acc[...] + second(False)) * gain
    pl.delay(1)
    settle(rz.at[pl.ds(0, NZ - 1)], rrz)
    pl.delay(1)
    acc[:, OWN * BLK :] = acc[:, OWN * BLK :] + nugget * resid
    curve = jnp.zeros((RHS, BLK), F32)
    for o in range(NZ):
        curve = curve + acc[:, o * BLK : (o + 1) * BLK] * rz[o]
    curve = jnp.sum(curve, axis=1, keepdims=True)
    here_lane = lanes == lax.broadcasted_iota(jnp.int32, (RHS, BLK), 0)
    gf[f] = jnp.sum(jnp.where(here_lane, curve, 0.0), axis=0, keepdims=True)
    for _, _, device in plane[::-1]:
        send(gf.at[f], gf.at[f], sg, rg, device)
    for _, here, device in along_z:
        send(acc.at[:, here * BLK : (here + 1) * BLK], fr.at[z], ss, rs, device)
    fr[z] = acc[:, OWN * BLK :]
    pl.delay(1)
    settle(gf.at[pl.ds(0, NF - 1)], rg)
    pl.delay(1)
    hz[z] = jnp.sum(gf[...], axis=0)
    for _, _, device in along_z:
        send(hz.at[z], hz.at[z], sh, rh, device)
    pl.delay(1)
    settle(tf.at[pl.ds(0, NF - 1)], rt)
    stats = jnp.sum(tf[...], axis=0)
    beta = matmul(stats[:, 0:RITZ], inverse, ((1,), (0,)))
    shift = matmul(beta, wide, ((1,), (0,)))
    direction = resid - shift[:, 0:BLK]
    deflated = jnp.sum(stats[:, 0:RITZ] * beta, axis=1, keepdims=True)
    settle(fr.at[pl.ds(0, NZ - 1)], rs)
    applied = jnp.sum(fr[...], axis=0) - shift[:, BLK:]
    pl.delay(1)
    settle(hz.at[pl.ds(0, NZ - 1)], rh)
    pl.delay(1)
    curve = jnp.sum(jnp.where(here_lane, jnp.sum(hz[...], axis=0), 0.0), axis=1, keepdims=True) - deflated
    step = stats[:, RITZ : RITZ + 1] / curve
    out_ref[0:RHS] = sol + step * direction
    out_ref[RHS:] = resid - step * applied

    pl.delay(1)
    settle(xf.at[0, pl.ds(0, CHIPS - 1)], sx)
    settle(xf.at[0], sxf)
    settle(xz.at[pl.ds(0, NZ - 1)], sxz)
    settle(vf.at[0, pl.ds(0, CHIPS - 1)], sv)
    for o in range(2):
        settle(vf.at[0, pl.ds(0, HERE)], svf.at[o])
    settle(wz.at[:, pl.ds(0, (NZ - 1) * BLK)], sw)
    settle(pin.at[pl.ds(0, NZ - 1)], sp)
    settle(ara.at[pl.ds(0, NZ - 1)], sa)
    settle(arb.at[pl.ds(0, NF - 1)], sb)
    settle(arc.at[pl.ds(0, NZ - 1)], sc)
    settle(rf.at[0, pl.ds(0, CHIPS - 1)], sr)
    settle(rf.at[1], sr)
    settle(rz.at[pl.ds(0, NZ - 1)], srz)
    settle(tz.at[pl.ds(0, NZ - 1)], stz)
    settle(fr.at[pl.ds(0, NZ - 1)], ss)
    settle(tf.at[pl.ds(0, NF - 1)], st)
    settle(gf.at[pl.ds(0, NF - 1)], sg)
    settle(hz.at[pl.ds(0, NZ - 1)], sh)


def local(points, inv_scales, amplitude, noise_var, targets, initial, ritz_basis):
    dma = pltpu.SemaphoreType.DMA
    hbm = pl.BlockSpec(memory_space=pltpu.HBM)
    vmem = pl.BlockSpec(memory_space=pltpu.VMEM)
    both = pl.pallas_call(
        body,
        out_shape=pltpu.VMEM((2 * RHS, BLK), F32),
        in_specs=[hbm, hbm, hbm, hbm, hbm, hbm, hbm],
        out_specs=vmem,
        scratch_shapes=[
            pltpu.SMEM((1,), F32),
            pltpu.SMEM((1,), F32),
            pltpu.SMEM((FEAT,), F32),
            pltpu.VMEM((FEAT, BLK), F32),
            pltpu.VMEM((NC, CHIPS, FEAT, BLK), F32),
            pltpu.VMEM((NZ, FEAT, BLK), F32),
            pltpu.VMEM((NC, CHIPS, VEC, BLK), F32),
            pltpu.VMEM((RITZ, NI), F32),
            pltpu.VMEM((RHS, BLK), F32),
            pltpu.VMEM((NJ, BLK), BF16),
            pltpu.VMEM((BLK, NI), BF16),
            pltpu.VMEM((NJ, NI), BF16),
            pltpu.VMEM((NJ, NI), BF16),
            pltpu.VMEM((2 * PAD, NJ), BF16),
            pltpu.VMEM((VEC, NI), F32),
            pltpu.VMEM((NZ, VEC, BLK), F32),
            pltpu.VMEM((NZ, RHS, BLK), F32),
            pltpu.VMEM((NZ, RHS, BLK), F32),
            pltpu.VMEM((NF, RHS, BLK), F32),
            pltpu.VMEM((NZ, RHS, BLK), F32),
            pltpu.VMEM((NC, CHIPS, RHS, BLK), F32),
            pltpu.VMEM((NZ, RHS, BLK), F32),
            pltpu.VMEM((NZ, RHS, BLK), F32),
            pltpu.VMEM((NF, RHS, BLK), F32),
            pltpu.VMEM((RHS, NI), F32),
            pltpu.VMEM((NZ, RHS, BLK), F32),
            pltpu.VMEM((NF, 1, BLK), F32),
            pltpu.VMEM((NZ, 1, BLK), F32),
            dma((8,)), dma, dma, dma, dma((2,)), dma((2,)), dma, dma, dma, dma, dma, dma((2,)), dma, dma, dma, dma, dma, dma,
            dma, dma, dma, dma, dma((2,)), dma, dma, dma, dma, dma, dma, dma, dma, dma, dma, dma, dma,
        ],
        compiler_params=pltpu.CompilerParams(
            collective_id=0, has_side_effects=True, vmem_limit_bytes=60 * 1024 * 1024
        ),
    )(amplitude, noise_var, inv_scales, points, targets, initial, ritz_basis)
    return both[:RHS], both[RHS:]


def solution(mesh):
    torus = Mesh(mesh.devices.reshape(NY, NZ, NX, NC), ("row_0", "row_1", "col_0", "col_1"))
    split = P(None, ("col_0", "col_1", "row_0", "row_1"))
    return jax.shard_map(
        local,
        mesh=torus,
        in_specs=(split, P(), P(), P(), split, split, split),
        out_specs=(split, split),
        check_vma=False,
    )
```

```python
import functools
import math

import jax
import jax.numpy as jnp
from jax import lax
from jax.experimental import pallas as pl
from jax.experimental.pallas import tpu as pltpu
from jax.sharding import Mesh
from jax.sharding import PartitionSpec as P

F32 = jnp.float32
BF16 = jnp.bfloat16
HIGH = lax.Precision.HIGHEST
MESH = pl.DeviceIdType.MESH
NY, NZ, NX, NC = 4, 8, 4, 2
CHIPS = NX * NY
NF = CHIPS * NC
BLK = 128
FEAT = 16
RITZ = 64
RHS = 8
VEC = RITZ + RHS
PAD = 80
NJ = NF * BLK
HALF = CHIPS * BLK
ROWS = 1024
NI = NZ * BLK
NEAR = sorted(((a, b) for a in range(NX) for b in range(NY)), key=lambda o: (min(o[0], NX - o[0]) + min(o[1], NY - o[1]), o))
HERE = CHIPS // 2
FAR = (4, 3, 5, 2, 6, 1, 7, 0)
OWN = NZ - 1
LOG2E = 1.4426950408889634


def split3(a):
    high = a.astype(BF16).astype(F32)
    rest = a - high
    mid = rest.astype(BF16).astype(F32)
    low = (rest - mid).astype(BF16).astype(F32)
    return high, mid, low


def matmul(a, b, dims):
    return lax.dot_general(a, b, (dims, ((), ())), precision=HIGH, preferred_element_type=F32)


def fast(a, b):
    return jnp.dot(a, b, preferred_element_type=F32)


def features(y, left):
    h, m, low = split3(y)
    sh, sm, sl = split3(-0.5 * jnp.sum(y * y, axis=0, keepdims=True))
    row = lax.broadcasted_iota(jnp.int32, (FEAT, BLK), 0)
    at = 0 if left else 3
    ones = (row < 6) & ((row >= 3) if left else (row < 3))
    extra = jnp.where(row == at, sh, jnp.where(row == at + 1, sm, jnp.where(row == at + 2, sl, 0.0)))
    extra = jnp.where(ones, 1.0, extra)
    zero = jnp.zeros((FEAT, BLK), F32)
    parts = [h, m, h, low, h, m, extra, zero] if left else [h, h, m, h, low, m, extra, zero]
    return jnp.concatenate(parts, axis=0)


def inverse2(m):
    a, b, e, d = m
    r = 1.0 / (a * d - b * e)
    return d * r, -b * r, -e * r, a * r


def multiply2(m, n):
    return (
        m[0] * n[0] + m[1] * n[2],
        m[0] * n[1] + m[1] * n[3],
        m[2] * n[0] + m[3] * n[2],
        m[2] * n[1] + m[3] * n[3],
    )


def eliminate(work):
    def full(a):
        return jnp.broadcast_to(a, (RHS, BLK))

    sub = lax.broadcasted_iota(jnp.int32, (RHS, BLK), 0)
    tiles = [work[RHS * i : RHS * (i + 1)] for i in range(RITZ // RHS)]
    for k in range(0, RITZ, 4):
        v, r = k // RHS, k % RHS
        cols = [[full(t[:, RITZ + k + j : RITZ + k + j + 1]) for t in tiles] for j in range(4)]
        u = [full(tiles[v][r + i : r + i + 1]) for i in range(4)]
        m = [[full(cols[j][v][r + i : r + i + 1]) for j in range(4)] for i in range(4)]
        b = (m[0][2], m[0][3], m[1][2], m[1][3])
        first = inverse2((m[0][0], m[0][1], m[1][0], m[1][1]))
        low = multiply2((m[2][0], m[2][1], m[3][0], m[3][1]), first)
        schur = tuple(p - q for p, q in zip((m[2][2], m[2][3], m[3][2], m[3][3]), multiply2(low, b)))
        second = inverse2(schur)
        t2 = u[2] - low[0] * u[0] - low[1] * u[1]
        t3 = u[3] - low[2] * u[0] - low[3] * u[1]
        n2 = second[0] * t2 + second[1] * t3
        n3 = second[2] * t2 + second[3] * t3
        t0 = u[0] - b[0] * n2 - b[1] * n3
        t1 = u[1] - b[2] * n2 - b[3] * n3
        n0 = first[0] * t0 + first[1] * t1
        n1 = first[2] * t0 + first[3] * t1
        for j in range(4):
            cols[j][v] = jnp.where(sub == r + j, cols[j][v] - 1.0, cols[j][v])
        tiles = [
            t - (cols[0][i] * n0 + cols[1][i] * n1) - (cols[2][i] * n2 + cols[3][i] * n3)
            for i, t in enumerate(tiles)
        ]
    return jnp.concatenate(tiles, axis=0)


def body(
    gain_ref, nugget_ref, scales_ref, points_ref, targets_ref, initial_ref, ritz_ref, out_ref,
    gain_at, nugget_at, scales_at, px, xf, xz, vf, wz, tgt, ljt, riz, khi, klo, vcat, part, pin, ars, ara, arb, arc, rf, rz, tz, tf, acc, fr, gf, hz,
    sem_in, rx, rxf, rxz, rv, rvf, rw, rp, ra, rb, rc, rr, rrz, rtz, rt, rs, rg, rh,
    sx, sxf, sxz, sv, svf, sw, sp, sa, sb, sc, sr, srz, stz, st, ss, sg, sh,
):
    y = lax.axis_index("row_0")
    z = lax.axis_index("row_1")
    x = lax.axis_index("col_0")
    c = lax.axis_index("col_1")
    f = (x * NY + y) * NC + c
    xs = [lax.rem(x + k, NX) for k in range(NX)]
    ys = [lax.rem(y + k, NY) for k in range(NY)]
    zs = [lax.rem(z + k, NZ) for k in range(NZ)]
    other = {"row_0": y, "row_1": z, "col_0": x, "col_1": 1 - c}
    along_z = [
        (FAR.index((NZ - k) % NZ), i, {"row_0": y, "row_1": zs[k], "col_0": x, "col_1": c}) for i, k in enumerate(FAR[:-1])
    ]

    def chip(k):
        return {"row_0": ys[NEAR[k][1]], "row_1": z, "col_0": xs[NEAR[k][0]]}

    plane = [(k, o, {**chip(k), "col_1": 1 - c if o else c}) for k in range(CHIPS) for o in (0, 1) if k or o]
    same_core = [(k, device) for k, o, device in plane if not o]
    def send(src, dst, sent, arrived, device):
        pltpu.make_async_remote_copy(
            src_ref=src, dst_ref=dst, send_sem=sent, recv_sem=arrived, device_id=device, device_id_type=MESH
        ).start()

    def settle(ref, sem):
        pltpu.make_async_copy(ref, ref, sem).wait()

    loads = [
        pltpu.make_async_copy(scales_ref, scales_at, sem_in.at[5]),
        pltpu.make_async_copy(gain_ref, gain_at, sem_in.at[6]),
        pltpu.make_async_copy(nugget_ref, nugget_at, sem_in.at[7]),
        pltpu.make_async_copy(points_ref, px, sem_in.at[0]),
        pltpu.make_async_copy(ritz_ref, vf.at[0, 0, pl.ds(0, RITZ)], sem_in.at[1]),
        pltpu.make_async_copy(initial_ref, vf.at[0, 0, pl.ds(RITZ, RHS)], sem_in.at[2]),
        pltpu.make_async_copy(targets_ref, tgt, sem_in.at[3]),
        pltpu.make_async_copy(ritz_ref, wz.at[:, OWN * BLK :], sem_in.at[4]),
    ]
    for load in loads:
        load.start()
    barrier = pltpu.get_barrier_semaphore()
    for device in [d for _, _, d in along_z] + [d for _, _, d in plane[::-1]]:
        pl.semaphore_signal(barrier, inc=1, device_id=device, device_id_type=MESH)

    row = lax.broadcasted_iota(jnp.int32, (FEAT, BLK), 0)
    for load in loads[:4]:
        load.wait()
    gain = gain_at[0]
    nugget = nugget_at[0]
    scale = jnp.zeros((FEAT, BLK), F32)
    for i in range(FEAT):
        scale = jnp.where(row == i, scales_at[i], scale)
    scaled = px[...] * scale * math.sqrt(LOG2E)
    xf[0, 0] = scaled
    xz[OWN] = scaled
    for load in loads[4:]:
        load.wait()
    pl.delay(1)
    pl.semaphore_wait(barrier, NF - 1 + NZ - 1)

    pl.delay(1)
    for there, _, device in along_z:
        send(xz.at[OWN], xz.at[there], sxz, rxz, device)
    for k, device in same_core:
        send(xf.at[0, 0], xf.at[0, k], sx, rx, device)
    own_vec = vf.at[0, 0]
    own_w = wz.at[:, OWN * BLK :]

    def bulk():
        for k, device in same_core:
            send(own_vec, vf.at[0, k], sv, rv.at[k // HERE], device)
        for there, _, device in along_z:
            send(own_w, wz.at[:, there * BLK : (there + 1) * BLK], sw, rw, device)

    bulk()
    pl.delay(1)
    settle(xf.at[0, pl.ds(0, CHIPS - 1)], rx)
    send(xf.at[0], xf.at[1], sxf, rxf, other)

    def side(h):
        for k in range(CHIPS):
            at = (h * CHIPS + k) * BLK
            ljt[at : at + BLK, :] = features(xf[h, k], True).T.astype(BF16)

    def tile_rows(i):
        at = pl.ds(i * ROWS, ROWS)
        for to in (pl.ds(0, NI // 2), pl.ds(NI // 2, NI // 2)):
            tile = jnp.exp2(jnp.minimum(fast(ljt[at, :], riz[:, to]), 0.0))
            high = tile.astype(BF16)
            khi[at, to] = high
            klo[at, to] = (tile - high.astype(F32)).astype(BF16)

    pl.delay(1)
    side(0)
    pl.delay(1)
    settle(xz.at[pl.ds(0, NZ - 1)], rxz)
    pl.delay(1)
    for o in range(NZ):
        riz[:, o * BLK : (o + 1) * BLK] = features(xz[o], False).astype(BF16)
    pl.delay(1)
    tile_rows(0)
    tile_rows(1)
    pl.delay(1)
    settle(xf.at[1], rxf)
    pl.delay(1)
    side(1)
    pl.delay(1)
    tile_rows(2)
    pl.delay(1)
    settle(vf.at[0, pl.ds(1, HERE - 1)], rv.at[0])
    send(vf.at[0, pl.ds(0, HERE)], vf.at[1, pl.ds(0, HERE)], svf.at[0], rvf.at[0], other)
    pl.delay(1)
    tile_rows(3)

    def vectors(h, near):
        for k in range(0 if near else HERE, HERE if near else CHIPS):
            high, mid, low = split3(vf[h, k])
            at = (h * CHIPS + k) * BLK
            v = jnp.concatenate([high, low[RITZ:], mid, jnp.zeros((PAD - VEC, BLK), F32)], axis=0)
            vcat[:, at : at + BLK] = v.astype(BF16)

    def product(h, near):
        vectors(h, near)
        at = pl.ds((h * CHIPS + (0 if near else HERE)) * BLK, HERE * BLK)
        a = fast(vcat[:, at], khi[at, :])
        b = fast(vcat[0:PAD, at], klo[at, :])
        low = jnp.concatenate([jnp.zeros((RITZ, NI), F32), a[VEC:PAD] + b[VEC:PAD]], axis=0)
        return a[0:VEC] + a[PAD : PAD + VEC] + b[0:VEC] + low

    pl.delay(1)
    part[...] = product(0, True)
    pl.delay(1)
    settle(vf.at[1, pl.ds(0, HERE)], rvf.at[0])
    pl.delay(1)
    part[...] = part[...] + product(1, True)
    pl.delay(1)
    settle(vf.at[0, pl.ds(HERE, HERE)], rv.at[1])
    send(vf.at[0, pl.ds(HERE, HERE)], vf.at[1, pl.ds(HERE, HERE)], svf.at[1], rvf.at[1], other)
    pl.delay(1)
    part[...] = part[...] + product(0, False)
    pl.delay(1)
    settle(vf.at[1, pl.ds(HERE, HERE)], rvf.at[1])
    pl.delay(1)
    part[...] = (part[...] + product(1, False)) * gain

    pl.delay(1)
    mine = part[:, OWN * BLK :] + nugget * own_vec[...]
    part[:, OWN * BLK :] = mine
    pin[z] = mine

    lane = lax.broadcasted_iota(jnp.int32, (RITZ, BLK), 1)
    pl.delay(1)
    settle(wz.at[:, pl.ds(0, (NZ - 1) * BLK)], rw)
    pl.delay(1)
    fill = jnp.zeros((BLK - VEC, NI), F32)
    coarse_part = matmul(wz[...], jnp.concatenate([part[...], fill], axis=0), ((1,), (1,)))
    ritz_own = own_vec[0:RITZ, :]
    start_own = own_vec[RITZ:VEC, :]
    target_rows = jnp.concatenate([jnp.zeros((RITZ, BLK), F32), tgt[...], jnp.zeros((BLK - VEC, BLK), F32)], axis=0)
    coarse_part = jnp.where(lane < RITZ, coarse_part, -coarse_part) + matmul(ritz_own, target_rows, ((1,), (1,)))
    ars[...] = coarse_part.reshape(NZ, RHS, BLK)
    for _, here, device in along_z:
        send(ars.at[zs[FAR[here]]], ara.at[z], sa, ra, device)
    for _, here, device in along_z:
        send(part.at[:, here * BLK : (here + 1) * BLK], pin.at[z], sp, rp, device)
    ara[z] = ars[z]
    pl.delay(1)
    settle(ara.at[pl.ds(0, NZ - 1)], ra)
    arb[f] = jnp.sum(ara[...], axis=0)
    for _, _, device in plane[::-1]:
        send(arb.at[f], arb.at[f], sb, rb, device)
    pl.delay(1)
    settle(arb.at[pl.ds(0, NF - 1)], rb)
    arc[z] = jnp.sum(arb[...], axis=0)
    for _, _, device in along_z:
        send(arc.at[z], arc.at[z], sc, rc, device)
    pl.delay(1)
    settle(arc.at[pl.ds(0, NZ - 1)], rc)
    pl.delay(1)
    first_sum = arc[...].reshape(RITZ, BLK)
    square = jnp.concatenate([first_sum, jnp.zeros((BLK - RITZ, BLK), F32)], axis=0)
    turned = square.T
    coarse = 0.5 * (first_sum + turned[0:RITZ])
    projected = turned[RITZ:VEC, 0:RITZ]
    sub = lax.broadcasted_iota(jnp.int32, (RITZ, BLK), 0)
    work = jnp.where(lane < RITZ, jnp.where(lane == sub, 1.0, 0.0), pltpu.roll(coarse, RITZ, 1))
    work = eliminate(work)
    inverse = work[:, 0:RITZ]
    pl.delay(1)
    amounts = matmul(projected, inverse, ((1,), (0,)))
    pl.delay(1)
    settle(pin.at[pl.ds(0, NZ - 1)], rp)
    image = jnp.sum(pin[...], axis=0)
    zimg = image[0:RITZ]
    r0 = tgt[...] - image[RITZ:VEC]
    pl.delay(1)
    wide = jnp.concatenate([ritz_own, zimg], axis=1)
    moved = matmul(amounts, wide, ((1,), (0,)))
    resid = r0 - moved[:, BLK:]
    rf[0] = resid
    rz[OWN] = resid

    pl.delay(1)
    for k, o, device in plane[::-1]:
        send(rf.at[0], rf.at[o * CHIPS + k], sr, rr, device)
    for there, _, device in along_z:
        send(rz.at[OWN], rz.at[there], srz, rrz, device)
    pl.delay(1)
    sol = start_own + moved[:, 0:BLK]
    lanes = lax.broadcasted_iota(jnp.int32, (RHS, BLK), 1)
    tall = jnp.concatenate([zimg, jnp.zeros((BLK - RITZ, BLK), F32)], axis=0)
    against = matmul(resid, tall, ((1,), (1,)))
    norm = jnp.sum(resid * resid, axis=1, keepdims=True)
    tz[z] = jnp.where(lanes < RITZ, against, jnp.where(lanes == RITZ, norm, 0.0))
    for _, _, device in along_z:
        send(tz.at[z], tz.at[z], stz, rtz, device)

    pl.delay(1)
    settle(rf.at[pl.ds(0, NF - 1)], rr)
    pl.delay(1)
    high, mid, low = split3(jnp.concatenate([rf[k] for k in range(NF)], axis=1))
    v = jnp.concatenate([high, mid, low, jnp.zeros_like(high)], axis=0).astype(BF16)
    a = fast(v, khi[...])
    b = fast(v[0:16], klo[...])
    acc[...] = (a[0:8] + a[8:16] + a[16:24] + b[0:8] + b[8:16]) * gain
    pl.delay(1)
    settle(rz.at[pl.ds(0, NZ - 1)], rrz)
    pl.delay(1)
    acc[:, OWN * BLK :] = acc[:, OWN * BLK :] + nugget * resid
    curve = jnp.zeros((RHS, BLK), F32)
    for o in range(NZ):
        curve = curve + acc[:, o * BLK : (o + 1) * BLK] * rz[o]
    curve = jnp.sum(curve, axis=1, keepdims=True)
    here_lane = lanes == lax.broadcasted_iota(jnp.int32, (RHS, BLK), 0)
    gf[f] = jnp.sum(jnp.where(here_lane, curve, 0.0), axis=0, keepdims=True)
    for _, _, device in plane[::-1]:
        send(gf.at[f], gf.at[f], sg, rg, device)
    for _, here, device in along_z:
        send(acc.at[:, here * BLK : (here + 1) * BLK], fr.at[z], ss, rs, device)
    fr[z] = acc[:, OWN * BLK :]
    pl.delay(1)
    settle(tz.at[pl.ds(0, NZ - 1)], rtz)
    tf[f] = jnp.sum(tz[...], axis=0)
    for _, _, device in plane[::-1]:
        send(tf.at[f], tf.at[f], st, rt, device)
    pl.delay(1)
    settle(gf.at[pl.ds(0, NF - 1)], rg)
    pl.delay(1)
    hz[z] = jnp.sum(gf[...], axis=0)
    for _, _, device in along_z:
        send(hz.at[z], hz.at[z], sh, rh, device)
    pl.delay(1)
    settle(tf.at[pl.ds(0, NF - 1)], rt)
    stats = jnp.sum(tf[...], axis=0)
    beta = matmul(stats[:, 0:RITZ], inverse, ((1,), (0,)))
    shift = matmul(beta, wide, ((1,), (0,)))
    direction = resid - shift[:, 0:BLK]
    deflated = jnp.sum(stats[:, 0:RITZ] * beta, axis=1, keepdims=True)
    settle(fr.at[pl.ds(0, NZ - 1)], rs)
    applied = jnp.sum(fr[...], axis=0) - shift[:, BLK:]
    pl.delay(1)
    settle(hz.at[pl.ds(0, NZ - 1)], rh)
    pl.delay(1)
    curve = jnp.sum(jnp.where(here_lane, jnp.sum(hz[...], axis=0), 0.0), axis=1, keepdims=True) - deflated
    step = stats[:, RITZ : RITZ + 1] / curve
    out_ref[0:RHS] = sol + step * direction
    out_ref[RHS:] = resid - step * applied

    pl.delay(1)
    settle(xf.at[0, pl.ds(0, CHIPS - 1)], sx)
    settle(xf.at[0], sxf)
    settle(xz.at[pl.ds(0, NZ - 1)], sxz)
    settle(vf.at[0, pl.ds(0, CHIPS - 1)], sv)
    for o in range(2):
        settle(vf.at[0, pl.ds(0, HERE)], svf.at[o])
    settle(wz.at[:, pl.ds(0, (NZ - 1) * BLK)], sw)
    settle(pin.at[pl.ds(0, NZ - 1)], sp)
    settle(ara.at[pl.ds(0, NZ - 1)], sa)
    settle(arb.at[pl.ds(0, NF - 1)], sb)
    settle(arc.at[pl.ds(0, NZ - 1)], sc)
    settle(rf.at[pl.ds(0, NF - 1)], sr)
    settle(rz.at[pl.ds(0, NZ - 1)], srz)
    settle(tz.at[pl.ds(0, NZ - 1)], stz)
    settle(fr.at[pl.ds(0, NZ - 1)], ss)
    settle(tf.at[pl.ds(0, NF - 1)], st)
    settle(gf.at[pl.ds(0, NF - 1)], sg)
    settle(hz.at[pl.ds(0, NZ - 1)], sh)


def local(points, inv_scales, amplitude, noise_var, targets, initial, ritz_basis):
    dma = pltpu.SemaphoreType.DMA
    hbm = pl.BlockSpec(memory_space=pltpu.HBM)
    vmem = pl.BlockSpec(memory_space=pltpu.VMEM)
    both = pl.pallas_call(
        body,
        out_shape=pltpu.VMEM((2 * RHS, BLK), F32),
        in_specs=[hbm, hbm, hbm, hbm, hbm, hbm, hbm],
        out_specs=vmem,
        scratch_shapes=[
            pltpu.SMEM((1,), F32),
            pltpu.SMEM((1,), F32),
            pltpu.SMEM((FEAT,), F32),
            pltpu.VMEM((FEAT, BLK), F32),
            pltpu.VMEM((NC, CHIPS, FEAT, BLK), F32),
            pltpu.VMEM((NZ, FEAT, BLK), F32),
            pltpu.VMEM((NC, CHIPS, VEC, BLK), F32),
            pltpu.VMEM((RITZ, NI), F32),
            pltpu.VMEM((RHS, BLK), F32),
            pltpu.VMEM((NJ, BLK), BF16),
            pltpu.VMEM((BLK, NI), BF16),
            pltpu.VMEM((NJ, NI), BF16),
            pltpu.VMEM((NJ, NI), BF16),
            pltpu.VMEM((2 * PAD, NJ), BF16),
            pltpu.VMEM((VEC, NI), F32),
            pltpu.VMEM((NZ, VEC, BLK), F32),
            pltpu.VMEM((NZ, RHS, BLK), F32),
            pltpu.VMEM((NZ, RHS, BLK), F32),
            pltpu.VMEM((NF, RHS, BLK), F32),
            pltpu.VMEM((NZ, RHS, BLK), F32),
            pltpu.VMEM((NF, RHS, BLK), F32),
            pltpu.VMEM((NZ, RHS, BLK), F32),
            pltpu.VMEM((NZ, RHS, BLK), F32),
            pltpu.VMEM((NF, RHS, BLK), F32),
            pltpu.VMEM((RHS, NI), F32),
            pltpu.VMEM((NZ, RHS, BLK), F32),
            pltpu.VMEM((NF, 1, BLK), F32),
            pltpu.VMEM((NZ, 1, BLK), F32),
            dma((8,)), dma, dma, dma, dma((2,)), dma((2,)), dma, dma, dma, dma, dma, dma, dma, dma, dma, dma, dma, dma,
            dma, dma, dma, dma, dma((2,)), dma, dma, dma, dma, dma, dma, dma, dma, dma, dma, dma, dma,
        ],
        compiler_params=pltpu.CompilerParams(
            collective_id=0, has_side_effects=True, vmem_limit_bytes=60 * 1024 * 1024
        ),
    )(amplitude, noise_var, inv_scales, points, targets, initial, ritz_basis)
    return both[:RHS], both[RHS:]


def solution(mesh):
    torus = Mesh(mesh.devices.reshape(NY, NZ, NX, NC), ("row_0", "row_1", "col_0", "col_1"))
    split = P(None, ("col_0", "col_1", "row_0", "row_1"))
    return jax.shard_map(
        local,
        mesh=torus,
        in_specs=(split, P(), P(), P(), split, split, split),
        out_specs=(split, split),
        check_vma=False,
    )
```

```python
import functools
import math

import jax
import jax.numpy as jnp
from jax import lax
from jax.experimental import pallas as pl
from jax.experimental.pallas import tpu as pltpu
from jax.sharding import Mesh
from jax.sharding import PartitionSpec as P

F32 = jnp.float32
BF16 = jnp.bfloat16
HIGH = lax.Precision.HIGHEST
MESH = pl.DeviceIdType.MESH
NY, NZ, NX, NC = 4, 8, 4, 2
CHIPS = NX * NY
NF = CHIPS * NC
BLK = 128
FEAT = 16
RITZ = 64
RHS = 8
VEC = RITZ + RHS
PAD = 80
NJ = NF * BLK
HALF = CHIPS * BLK
ROWS = 1024
NI = NZ * BLK
NEAR = sorted(((a, b) for a in range(NX) for b in range(NY)), key=lambda o: (min(o[0], NX - o[0]) + min(o[1], NY - o[1]), o))
HERE = CHIPS // 2
FIRST = 10
LAST = CHIPS - FIRST
FAR = (4, 3, 5, 2, 6, 1, 7, 0)
OWN = NZ - 1
LOG2E = 1.4426950408889634


def split3(a):
    high = a.astype(BF16).astype(F32)
    rest = a - high
    mid = rest.astype(BF16).astype(F32)
    low = (rest - mid).astype(BF16).astype(F32)
    return high, mid, low


def matmul(a, b, dims):
    return lax.dot_general(a, b, (dims, ((), ())), precision=HIGH, preferred_element_type=F32)


def fast(a, b):
    return jnp.dot(a, b, preferred_element_type=F32)


def features(y, left):
    h, m, low = split3(y)
    sh, sm, sl = split3(-0.5 * jnp.sum(y * y, axis=0, keepdims=True))
    row = lax.broadcasted_iota(jnp.int32, (FEAT, BLK), 0)
    at = 0 if left else 3
    ones = (row < 6) & ((row >= 3) if left else (row < 3))
    extra = jnp.where(row == at, sh, jnp.where(row == at + 1, sm, jnp.where(row == at + 2, sl, 0.0)))
    extra = jnp.where(ones, 1.0, extra)
    zero = jnp.zeros((FEAT, BLK), F32)
    parts = [h, m, h, low, h, m, extra, zero] if left else [h, h, m, h, low, m, extra, zero]
    return jnp.concatenate(parts, axis=0)


def inverse2(m):
    a, b, e, d = m
    r = 1.0 / (a * d - b * e)
    return d * r, -b * r, -e * r, a * r


def multiply2(m, n):
    return (
        m[0] * n[0] + m[1] * n[2],
        m[0] * n[1] + m[1] * n[3],
        m[2] * n[0] + m[3] * n[2],
        m[2] * n[1] + m[3] * n[3],
    )


def eliminate(work):
    def full(a):
        return jnp.broadcast_to(a, (RHS, BLK))

    sub = lax.broadcasted_iota(jnp.int32, (RHS, BLK), 0)
    tiles = [work[RHS * i : RHS * (i + 1)] for i in range(RITZ // RHS)]
    for k in range(0, RITZ, 4):
        v, r = k // RHS, k % RHS
        cols = [[full(t[:, RITZ + k + j : RITZ + k + j + 1]) for t in tiles] for j in range(4)]
        u = [full(tiles[v][r + i : r + i + 1]) for i in range(4)]
        m = [[full(cols[j][v][r + i : r + i + 1]) for j in range(4)] for i in range(4)]
        b = (m[0][2], m[0][3], m[1][2], m[1][3])
        first = inverse2((m[0][0], m[0][1], m[1][0], m[1][1]))
        low = multiply2((m[2][0], m[2][1], m[3][0], m[3][1]), first)
        schur = tuple(p - q for p, q in zip((m[2][2], m[2][3], m[3][2], m[3][3]), multiply2(low, b)))
        second = inverse2(schur)
        t2 = u[2] - low[0] * u[0] - low[1] * u[1]
        t3 = u[3] - low[2] * u[0] - low[3] * u[1]
        n2 = second[0] * t2 + second[1] * t3
        n3 = second[2] * t2 + second[3] * t3
        t0 = u[0] - b[0] * n2 - b[1] * n3
        t1 = u[1] - b[2] * n2 - b[3] * n3
        n0 = first[0] * t0 + first[1] * t1
        n1 = first[2] * t0 + first[3] * t1
        for j in range(4):
            cols[j][v] = jnp.where(sub == r + j, cols[j][v] - 1.0, cols[j][v])
        tiles = [
            t - (cols[0][i] * n0 + cols[1][i] * n1) - (cols[2][i] * n2 + cols[3][i] * n3)
            for i, t in enumerate(tiles)
        ]
    return jnp.concatenate(tiles, axis=0)


def body(
    gain_ref, nugget_ref, scales_ref, points_ref, targets_ref, initial_ref, ritz_ref, out_ref,
    gain_at, nugget_at, scales_at, px, xf, xz, vf, wz, tgt, ljt, riz, khi, klo, vcat, part, pin, ars, ara, arb, arc, rf, rz, tz, tf, acc, fr, gf, hz,
    sem_in, rx, rxf, rxz, rv, rvf, rw, rp, ra, rb, rc, rr, rrz, rtz, rt, rs, rg, rh,
    sx, sxf, sxz, sv, svf, sw, sp, sa, sb, sc, sr, srz, stz, st, ss, sg, sh,
):
    y = lax.axis_index("row_0")
    z = lax.axis_index("row_1")
    x = lax.axis_index("col_0")
    c = lax.axis_index("col_1")
    f = (x * NY + y) * NC + c
    xs = [lax.rem(x + k, NX) for k in range(NX)]
    ys = [lax.rem(y + k, NY) for k in range(NY)]
    zs = [lax.rem(z + k, NZ) for k in range(NZ)]
    other = {"row_0": y, "row_1": z, "col_0": x, "col_1": 1 - c}
    along_z = [
        (FAR.index((NZ - k) % NZ), i, {"row_0": y, "row_1": zs[k], "col_0": x, "col_1": c}) for i, k in enumerate(FAR[:-1])
    ]

    def chip(k):
        return {"row_0": ys[NEAR[k][1]], "row_1": z, "col_0": xs[NEAR[k][0]]}

    plane = [(k, o, {**chip(k), "col_1": 1 - c if o else c}) for k in range(CHIPS) for o in (0, 1) if k or o]
    same_core = [(k, device) for k, o, device in plane if not o]
    def send(src, dst, sent, arrived, device):
        pltpu.make_async_remote_copy(
            src_ref=src, dst_ref=dst, send_sem=sent, recv_sem=arrived, device_id=device, device_id_type=MESH
        ).start()

    def settle(ref, sem):
        pltpu.make_async_copy(ref, ref, sem).wait()

    loads = [
        pltpu.make_async_copy(scales_ref, scales_at, sem_in.at[5]),
        pltpu.make_async_copy(gain_ref, gain_at, sem_in.at[6]),
        pltpu.make_async_copy(nugget_ref, nugget_at, sem_in.at[7]),
        pltpu.make_async_copy(points_ref, px, sem_in.at[0]),
        pltpu.make_async_copy(ritz_ref, vf.at[0, 0, pl.ds(0, RITZ)], sem_in.at[1]),
        pltpu.make_async_copy(initial_ref, vf.at[0, 0, pl.ds(RITZ, RHS)], sem_in.at[2]),
        pltpu.make_async_copy(targets_ref, tgt, sem_in.at[3]),
        pltpu.make_async_copy(ritz_ref, wz.at[:, OWN * BLK :], sem_in.at[4]),
    ]
    for load in loads:
        load.start()
    barrier = pltpu.get_barrier_semaphore()
    for device in [d for _, _, d in along_z] + [d for _, _, d in plane[::-1]]:
        pl.semaphore_signal(barrier, inc=1, device_id=device, device_id_type=MESH)

    row = lax.broadcasted_iota(jnp.int32, (FEAT, BLK), 0)
    for load in loads[:4]:
        load.wait()
    gain = gain_at[0]
    nugget = nugget_at[0]
    scale = jnp.zeros((FEAT, BLK), F32)
    for i in range(FEAT):
        scale = jnp.where(row == i, scales_at[i], scale)
    scaled = px[...] * scale * math.sqrt(LOG2E)
    xf[0, 0] = scaled
    xz[OWN] = scaled
    for load in loads[4:]:
        load.wait()
    pl.delay(1)
    pl.semaphore_wait(barrier, NF - 1 + NZ - 1)

    pl.delay(1)
    for there, _, device in along_z:
        send(xz.at[OWN], xz.at[there], sxz, rxz, device)
    for k, device in same_core:
        send(xf.at[0, 0], xf.at[0, k], sx, rx, device)
    own_vec = vf.at[0, 0]
    own_w = wz.at[:, OWN * BLK :]

    def bulk():
        for k, device in same_core:
            send(own_vec, vf.at[0, k], sv, rv.at[int(k >= FIRST)], device)
        for there, _, device in along_z:
            send(own_w, wz.at[:, there * BLK : (there + 1) * BLK], sw, rw, device)

    bulk()
    pl.delay(1)
    settle(xf.at[0, pl.ds(0, CHIPS - 1)], rx)
    send(xf.at[0], xf.at[1], sxf, rxf, other)

    def side(h):
        for k in range(CHIPS):
            at = (h * CHIPS + k) * BLK
            ljt[at : at + BLK, :] = features(xf[h, k], True).T.astype(BF16)

    def tile_rows(i):
        at = pl.ds(i * ROWS, ROWS)
        for to in (pl.ds(0, NI // 2), pl.ds(NI // 2, NI // 2)):
            tile = jnp.exp2(jnp.minimum(fast(ljt[at, :], riz[:, to]), 0.0))
            high = tile.astype(BF16)
            khi[at, to] = high
            klo[at, to] = (tile - high.astype(F32)).astype(BF16)

    pl.delay(1)
    side(0)
    pl.delay(1)
    settle(xz.at[pl.ds(0, NZ - 1)], rxz)
    pl.delay(1)
    for o in range(NZ):
        riz[:, o * BLK : (o + 1) * BLK] = features(xz[o], False).astype(BF16)
    pl.delay(1)
    tile_rows(0)
    tile_rows(1)
    pl.delay(1)
    settle(xf.at[1], rxf)
    pl.delay(1)
    side(1)
    pl.delay(1)
    tile_rows(2)
    pl.delay(1)
    settle(vf.at[0, pl.ds(1, FIRST - 1)], rv.at[0])
    send(vf.at[0, pl.ds(0, FIRST)], vf.at[1, pl.ds(0, FIRST)], svf.at[0], rvf.at[0], other)
    pl.delay(1)
    tile_rows(3)

    def vectors(h, near):
        for k in range(0 if near else FIRST, FIRST if near else CHIPS):
            high, mid, low = split3(vf[h, k])
            at = (h * CHIPS + k) * BLK
            v = jnp.concatenate([high, low[RITZ:], mid, jnp.zeros((PAD - VEC, BLK), F32)], axis=0)
            vcat[:, at : at + BLK] = v.astype(BF16)

    def product(h, near):
        vectors(h, near)
        at = pl.ds((h * CHIPS + (0 if near else FIRST)) * BLK, (FIRST if near else LAST) * BLK)
        a = fast(vcat[:, at], khi[at, :])
        b = fast(vcat[0:PAD, at], klo[at, :])
        low = jnp.concatenate([jnp.zeros((RITZ, NI), F32), a[VEC:PAD] + b[VEC:PAD]], axis=0)
        return a[0:VEC] + a[PAD : PAD + VEC] + b[0:VEC] + low

    pl.delay(1)
    part[...] = product(0, True)
    pl.delay(1)
    settle(vf.at[1, pl.ds(0, FIRST)], rvf.at[0])
    pl.delay(1)
    part[...] = part[...] + product(1, True)
    pl.delay(1)
    settle(vf.at[0, pl.ds(FIRST, LAST)], rv.at[1])
    send(vf.at[0, pl.ds(FIRST, LAST)], vf.at[1, pl.ds(FIRST, LAST)], svf.at[1], rvf.at[1], other)
    pl.delay(1)
    part[...] = part[...] + product(0, False)
    pl.delay(1)
    settle(vf.at[1, pl.ds(FIRST, LAST)], rvf.at[1])
    pl.delay(1)
    part[...] = (part[...] + product(1, False)) * gain

    pl.delay(1)
    mine = part[:, OWN * BLK :] + nugget * own_vec[...]
    part[:, OWN * BLK :] = mine
    pin[z] = mine

    lane = lax.broadcasted_iota(jnp.int32, (RITZ, BLK), 1)
    pl.delay(1)
    settle(wz.at[:, pl.ds(0, (NZ - 1) * BLK)], rw)
    pl.delay(1)
    fill = jnp.zeros((BLK - VEC, NI), F32)
    coarse_part = matmul(wz[...], jnp.concatenate([part[...], fill], axis=0), ((1,), (1,)))
    ritz_own = own_vec[0:RITZ, :]
    start_own = own_vec[RITZ:VEC, :]
    target_rows = jnp.concatenate([jnp.zeros((RITZ, BLK), F32), tgt[...], jnp.zeros((BLK - VEC, BLK), F32)], axis=0)
    coarse_part = jnp.where(lane < RITZ, coarse_part, -coarse_part) + matmul(ritz_own, target_rows, ((1,), (1,)))
    ars[...] = coarse_part.reshape(NZ, RHS, BLK)
    for _, here, device in along_z:
        send(ars.at[zs[FAR[here]]], ara.at[z], sa, ra, device)
    for _, here, device in along_z:
        send(part.at[:, here * BLK : (here + 1) * BLK], pin.at[z], sp, rp, device)
    ara[z] = ars[z]
    pl.delay(1)
    settle(ara.at[pl.ds(0, NZ - 1)], ra)
    arb[f] = jnp.sum(ara[...], axis=0)
    for _, _, device in plane[::-1]:
        send(arb.at[f], arb.at[f], sb, rb, device)
    pl.delay(1)
    settle(arb.at[pl.ds(0, NF - 1)], rb)
    arc[z] = jnp.sum(arb[...], axis=0)
    for _, _, device in along_z:
        send(arc.at[z], arc.at[z], sc, rc, device)
    pl.delay(1)
    settle(arc.at[pl.ds(0, NZ - 1)], rc)
    pl.delay(1)
    first_sum = arc[...].reshape(RITZ, BLK)
    square = jnp.concatenate([first_sum, jnp.zeros((BLK - RITZ, BLK), F32)], axis=0)
    turned = square.T
    coarse = 0.5 * (first_sum + turned[0:RITZ])
    projected = turned[RITZ:VEC, 0:RITZ]
    sub = lax.broadcasted_iota(jnp.int32, (RITZ, BLK), 0)
    work = jnp.where(lane < RITZ, jnp.where(lane == sub, 1.0, 0.0), pltpu.roll(coarse, RITZ, 1))
    work = eliminate(work)
    inverse = work[:, 0:RITZ]
    pl.delay(1)
    amounts = matmul(projected, inverse, ((1,), (0,)))
    pl.delay(1)
    settle(pin.at[pl.ds(0, NZ - 1)], rp)
    image = jnp.sum(pin[...], axis=0)
    zimg = image[0:RITZ]
    r0 = tgt[...] - image[RITZ:VEC]
    pl.delay(1)
    wide = jnp.concatenate([ritz_own, zimg], axis=1)
    moved = matmul(amounts, wide, ((1,), (0,)))
    resid = r0 - moved[:, BLK:]
    rf[0, 0] = resid
    rz[OWN] = resid

    pl.delay(1)
    for k, o, device in plane[::-1]:
        send(rf.at[0, 0], rf.at[o, k], sr, rr.at[k // HERE], device)
    for there, _, device in along_z:
        send(rz.at[OWN], rz.at[there], srz, rrz, device)
    pl.delay(1)
    sol = start_own + moved[:, 0:BLK]
    lanes = lax.broadcasted_iota(jnp.int32, (RHS, BLK), 1)
    tall = jnp.concatenate([zimg, jnp.zeros((BLK - RITZ, BLK), F32)], axis=0)
    against = matmul(resid, tall, ((1,), (1,)))
    norm = jnp.sum(resid * resid, axis=1, keepdims=True)
    tz[z] = jnp.where(lanes < RITZ, against, jnp.where(lanes == RITZ, norm, 0.0))
    for _, _, device in along_z:
        send(tz.at[z], tz.at[z], stz, rtz, device)

    def second(near):
        total = None
        for h in range(NC):
            slots = range(0 if near else HERE, HERE if near else CHIPS)
            high, mid, low = split3(jnp.concatenate([rf[h, k] for k in slots], axis=1))
            v = jnp.concatenate([high, mid, low, jnp.zeros_like(high)], axis=0).astype(BF16)
            at = pl.ds((h * CHIPS + slots[0]) * BLK, HERE * BLK)
            a = fast(v, khi[at, :])
            b = fast(v[0:16], klo[at, :])
            one = a[0:8] + a[8:16] + a[16:24] + b[0:8] + b[8:16]
            total = one if total is None else total + one
        return total

    pl.delay(1)
    settle(rf.at[0, pl.ds(0, 2 * HERE - 1)], rr.at[0])
    pl.delay(1)
    acc[...] = second(True)
    pl.delay(1)
    settle(rf.at[:, pl.ds(HERE, HERE)], rr.at[1])
    pl.delay(1)
    acc[...] = (acc[...] + second(False)) * gain
    pl.delay(1)
    settle(rz.at[pl.ds(0, NZ - 1)], rrz)
    pl.delay(1)
    acc[:, OWN * BLK :] = acc[:, OWN * BLK :] + nugget * resid
    curve = jnp.zeros((RHS, BLK), F32)
    for o in range(NZ):
        curve = curve + acc[:, o * BLK : (o + 1) * BLK] * rz[o]
    curve = jnp.sum(curve, axis=1, keepdims=True)
    here_lane = lanes == lax.broadcasted_iota(jnp.int32, (RHS, BLK), 0)
    gf[f] = jnp.sum(jnp.where(here_lane, curve, 0.0), axis=0, keepdims=True)
    for _, _, device in plane[::-1]:
        send(gf.at[f], gf.at[f], sg, rg, device)
    for _, here, device in along_z:
        send(acc.at[:, here * BLK : (here + 1) * BLK], fr.at[z], ss, rs, device)
    fr[z] = acc[:, OWN * BLK :]
    pl.delay(1)
    settle(tz.at[pl.ds(0, NZ - 1)], rtz)
    tf[f] = jnp.sum(tz[...], axis=0)
    for _, _, device in plane[::-1]:
        send(tf.at[f], tf.at[f], st, rt, device)
    pl.delay(1)
    settle(gf.at[pl.ds(0, NF - 1)], rg)
    pl.delay(1)
    hz[z] = jnp.sum(gf[...], axis=0)
    for _, _, device in along_z:
        send(hz.at[z], hz.at[z], sh, rh, device)
    pl.delay(1)
    settle(tf.at[pl.ds(0, NF - 1)], rt)
    stats = jnp.sum(tf[...], axis=0)
    beta = matmul(stats[:, 0:RITZ], inverse, ((1,), (0,)))
    shift = matmul(beta, wide, ((1,), (0,)))
    direction = resid - shift[:, 0:BLK]
    deflated = jnp.sum(stats[:, 0:RITZ] * beta, axis=1, keepdims=True)
    settle(fr.at[pl.ds(0, NZ - 1)], rs)
    applied = jnp.sum(fr[...], axis=0) - shift[:, BLK:]
    pl.delay(1)
    settle(hz.at[pl.ds(0, NZ - 1)], rh)
    pl.delay(1)
    curve = jnp.sum(jnp.where(here_lane, jnp.sum(hz[...], axis=0), 0.0), axis=1, keepdims=True) - deflated
    step = stats[:, RITZ : RITZ + 1] / curve
    out_ref[0:RHS] = sol + step * direction
    out_ref[RHS:] = resid - step * applied

    pl.delay(1)
    settle(xf.at[0, pl.ds(0, CHIPS - 1)], sx)
    settle(xf.at[0], sxf)
    settle(xz.at[pl.ds(0, NZ - 1)], sxz)
    settle(vf.at[0, pl.ds(0, CHIPS - 1)], sv)
    settle(vf.at[0, pl.ds(0, FIRST)], svf.at[0])
    settle(vf.at[0, pl.ds(0, LAST)], svf.at[1])
    settle(wz.at[:, pl.ds(0, (NZ - 1) * BLK)], sw)
    settle(pin.at[pl.ds(0, NZ - 1)], sp)
    settle(ara.at[pl.ds(0, NZ - 1)], sa)
    settle(arb.at[pl.ds(0, NF - 1)], sb)
    settle(arc.at[pl.ds(0, NZ - 1)], sc)
    settle(rf.at[0, pl.ds(0, CHIPS - 1)], sr)
    settle(rf.at[1], sr)
    settle(rz.at[pl.ds(0, NZ - 1)], srz)
    settle(tz.at[pl.ds(0, NZ - 1)], stz)
    settle(fr.at[pl.ds(0, NZ - 1)], ss)
    settle(tf.at[pl.ds(0, NF - 1)], st)
    settle(gf.at[pl.ds(0, NF - 1)], sg)
    settle(hz.at[pl.ds(0, NZ - 1)], sh)


def local(points, inv_scales, amplitude, noise_var, targets, initial, ritz_basis):
    dma = pltpu.SemaphoreType.DMA
    hbm = pl.BlockSpec(memory_space=pltpu.HBM)
    vmem = pl.BlockSpec(memory_space=pltpu.VMEM)
    both = pl.pallas_call(
        body,
        out_shape=pltpu.VMEM((2 * RHS, BLK), F32),
        in_specs=[hbm, hbm, hbm, hbm, hbm, hbm, hbm],
        out_specs=vmem,
        scratch_shapes=[
            pltpu.SMEM((1,), F32),
            pltpu.SMEM((1,), F32),
            pltpu.SMEM((FEAT,), F32),
            pltpu.VMEM((FEAT, BLK), F32),
            pltpu.VMEM((NC, CHIPS, FEAT, BLK), F32),
            pltpu.VMEM((NZ, FEAT, BLK), F32),
            pltpu.VMEM((NC, CHIPS, VEC, BLK), F32),
            pltpu.VMEM((RITZ, NI), F32),
            pltpu.VMEM((RHS, BLK), F32),
            pltpu.VMEM((NJ, BLK), BF16),
            pltpu.VMEM((BLK, NI), BF16),
            pltpu.VMEM((NJ, NI), BF16),
            pltpu.VMEM((NJ, NI), BF16),
            pltpu.VMEM((2 * PAD, NJ), BF16),
            pltpu.VMEM((VEC, NI), F32),
            pltpu.VMEM((NZ, VEC, BLK), F32),
            pltpu.VMEM((NZ, RHS, BLK), F32),
            pltpu.VMEM((NZ, RHS, BLK), F32),
            pltpu.VMEM((NF, RHS, BLK), F32),
            pltpu.VMEM((NZ, RHS, BLK), F32),
            pltpu.VMEM((NC, CHIPS, RHS, BLK), F32),
            pltpu.VMEM((NZ, RHS, BLK), F32),
            pltpu.VMEM((NZ, RHS, BLK), F32),
            pltpu.VMEM((NF, RHS, BLK), F32),
            pltpu.VMEM((RHS, NI), F32),
            pltpu.VMEM((NZ, RHS, BLK), F32),
            pltpu.VMEM((NF, 1, BLK), F32),
            pltpu.VMEM((NZ, 1, BLK), F32),
            dma((8,)), dma, dma, dma, dma((2,)), dma((2,)), dma, dma, dma, dma, dma, dma((2,)), dma, dma, dma, dma, dma, dma,
            dma, dma, dma, dma, dma((2,)), dma, dma, dma, dma, dma, dma, dma, dma, dma, dma, dma, dma,
        ],
        compiler_params=pltpu.CompilerParams(
            collective_id=0, has_side_effects=True, vmem_limit_bytes=60 * 1024 * 1024
        ),
    )(amplitude, noise_var, inv_scales, points, targets, initial, ritz_basis)
    return both[:RHS], both[RHS:]


def solution(mesh):
    torus = Mesh(mesh.devices.reshape(NY, NZ, NX, NC), ("row_0", "row_1", "col_0", "col_1"))
    split = P(None, ("col_0", "col_1", "row_0", "row_1"))
    return jax.shard_map(
        local,
        mesh=torus,
        in_specs=(split, P(), P(), P(), split, split, split),
        out_specs=(split, split),
        check_vma=False,
    )
```
